32 devices in a mesh: ta: 4 (over y, x), gz: 2 (over core), xy: 4 (over z).
Axes of the slice: x: 2, y: 2, z: 4, core: 2. Of those that a mesh axis runs over, the one named last changes fastest.
Arguments:
- source: float32 [2, 4, 3, 16, 16, 512], P(None, None, None, 'ta', 'gz', 'xy'), may hold values from -6 to 6
- iterate: float32 [2, 4, 3, 16, 16, 512], P(None, None, None, 'ta', 'gz', 'xy'), may hold values from -6 to 6
- gauge_links: float32 [4, 2, 3, 3, 16, 16, 512], P(None, None, None, None, 'ta', 'gz', 'xy'), may hold values from -2.4 to 2.4
- clover: float32 [2, 2, 6, 6, 16, 16, 512], P(None, None, None, None, 'ta', 'gz', 'xy'), may hold values from -0.6 to 0.6
- bc_sign: int32 [4], replicated, may hold values from -1 to 1, as said below
- null_store: bfloat16 [4, 4, 4, 2, 24, 12, 4, 4, 128], P('ta', 'gz', 'xy'), may hold values from -0.109375 to 0.109375
- block_slot: int32 [4, 4, 4], P('ta', 'gz', 'xy'), may hold values from 0 to 1, as said below
- coarse_links: float32 [9, 2, 24, 24, 4, 4, 4, 8], P(None, None, None, None, 'ta', 'gz', 'xy'), may hold values from -0.2 to 0.2
Outputs:
- new_iterate: float32 [2, 4, 3, 16, 16, 512], P(None, None, None, 'ta', 'gz', 'xy')
- new_residual: float32 [2, 4, 3, 16, 16, 512], P(None, None, None, 'ta', 'gz', 'xy')
The draws below stay inside these ranges and needn't reach their ends.
Inputs may be any that keep to these rules, and one draw needn't show every extreme that they name: `bc_sign`: each entry is -1 or +1. `block_slot`: within each device's block of 2 aggregate columns the entries are the numbers 0 to 1, each once.
All inputs are finite; a program needn't handle non-finite values.
Results may differ from the reference program's by a relative error of at most 0.0016.
Values sent between devices are 32-bit elements; how exact they have to be, the bound alone decides.
A program may use at most 256 MiB of HBM per device.

```python
import jax
import jax.numpy as jnp
import numpy as np
from jax import lax

NV = 24
BLK = 4
LT = 4
LZ = 8
LX = 4
LY = 32
CITERS = 4
NT = 16
NZ = 16
NXY = 512
CT = 4
CZ = 4
CX = 4
CY = 8


def draw_bc_sign(key, part):
    return 2 * jax.random.randint(key, (4,), 0, 2, dtype=jnp.int32) - 1


def draw_block_slot(key, part):
    dev_t = LT // BLK
    dev_z = LZ // BLK
    dev_x = LX // BLK
    count_t = CT // dev_t
    count_z = CZ // dev_z
    count_x = CX // dev_x
    per_device = dev_t * dev_z * dev_x
    scores = jax.random.randint(key, (count_t * count_z * count_x, per_device), 0, 1 << 16, dtype=jnp.int32)
    scores = scores * per_device + jnp.arange(per_device, dtype=jnp.int32)[None, :]
    ordering = jnp.argsort(scores, axis=1).astype(jnp.int32)
    ordering = ordering.reshape((count_t, count_z, count_x, dev_t, dev_z, dev_x))
    ordering = jnp.transpose(ordering, (0, 3, 1, 4, 2, 5))
    return ordering.reshape((CT, CZ, CX))


def level_of(own_key, shape, split, smallest, high):
    def one(dim, parts):
        draws = jax.random.uniform(jax.random.fold_in(jax.random.fold_in(own_key, 6), dim), (parts,), jnp.float32, smallest / len(split), high / len(split))
        return jnp.repeat(jnp.exp(draws), shape[dim] // parts).reshape((-1,) + (1,) * (len(shape) - dim - 1))

    loudness = one(*split[0])
    for cut in split[1:]:
        loudness = loudness * one(*cut)
    return loudness


def scatter_about(stream_key, shape, scale, bound, cuts=(), kind=jnp.bfloat16):
    values = scale * jax.random.normal(stream_key, shape, jnp.float32)
    if cuts:
        values = values * level_of(stream_key, shape, cuts, -0.22, 0.18)
    return jnp.clip(values, -bound, bound).astype(kind)


def setup_inputs(seed: int = 0) -> dict:
    key_list = jax.random.split(jax.random.key(seed), 9)
    source = scatter_about(key_list[0], (2, 4, 3, NT, NZ, NXY), 1.0, 6.0, ((3, 4), (4, 2), (5, 4)), jnp.float32)
    iterate = scatter_about(key_list[1], (2, 4, 3, NT, NZ, NXY), 1.0, 6.0, ((3, 4), (4, 2), (5, 4)), jnp.float32)
    gauge_links = scatter_about(key_list[2], (4, 2, 3, 3, NT, NZ, NXY), 0.4, 2.4, ((4, 4), (5, 2), (6, 4)), jnp.float32)
    clover = scatter_about(key_list[3], (2, 2, 6, 6, NT, NZ, NXY), 0.1, 0.6, ((4, 4), (5, 2), (6, 4)), jnp.float32)
    bc_sign = draw_bc_sign(jax.random.fold_in(key_list[8], 71), 0)
    null_store = scatter_about(key_list[5], (CT, CZ, CX, 2, NV, 12, BLK, BLK, BLK * LY), (12 * BLK ** 4) ** -0.5, 0.109375, ((0, 4), (1, 2), (2, 4)))
    block_slot = draw_block_slot(jax.random.fold_in(key_list[8], 71), 0)
    coarse_links = scatter_about(key_list[7], (9, 2, NV, NV, CT, CZ, CX, CY), 0.03, 0.2, ((4, 4), (5, 2), (6, 4)), jnp.float32)
    return {"source": source, "iterate": iterate, "gauge_links": gauge_links, "clover": clover, "bc_sign": bc_sign, "null_store": null_store, "block_slot": block_slot, "coarse_links": coarse_links}


MASS_TERM = 3.8
RELAX_WEIGHT = 0.4
HIGHEST = lax.Precision.HIGHEST


def chiral_blocks():
    identity = np.eye(2)
    nought = np.zeros((2, 2))
    flip_x = np.array([[0.0, 1.0], [1.0, 0.0]])
    flip_z = np.array([[1.0, 0.0], [0.0, -1.0]])
    rotate = np.array([[0.0, -1.0], [1.0, 0.0]])
    return [(identity, nought), (nought, -flip_z), (nought, -flip_x), (rotate, nought)]


def four_square(top_left, top_right, bottom_left, bottom_right):
    upper = np.concatenate([top_left, top_right], axis=1)
    lower = np.concatenate([bottom_left, bottom_right], axis=1)
    return np.concatenate([upper, lower], axis=0)


def spin_tables(direction, parity):
    upper_re, upper_im = chiral_blocks()[direction]
    identity = np.eye(2)
    nought = np.zeros((2, 2))
    gamma_re = four_square(nought, upper_re, upper_re.T, nought)
    gamma_im = four_square(nought, upper_im, -upper_im.T, nought)
    whole_re = np.eye(4) + parity * gamma_re
    whole_im = parity * gamma_im
    half_re = np.concatenate([identity, parity * upper_re], axis=1)
    half_im = np.concatenate([nought, parity * upper_im], axis=1)
    back_re = np.concatenate([identity, parity * upper_re.T], axis=0)
    back_im = np.concatenate([nought, -parity * upper_im.T], axis=0)
    return [np.asarray(matrix, np.float32) for matrix in (whole_re, whole_im, half_re, half_im, back_re, back_im)]


def spin_times(matrix_re, matrix_im, field):
    real_part = jnp.tensordot(matrix_re, field[0], axes=(1, 0), precision=HIGHEST) - jnp.tensordot(matrix_im, field[1], axes=(1, 0), precision=HIGHEST)
    imag_part = jnp.tensordot(matrix_re, field[1], axes=(1, 0), precision=HIGHEST) + jnp.tensordot(matrix_im, field[0], axes=(1, 0), precision=HIGHEST)
    return jnp.stack([real_part, imag_part])


def colour_times(link, field):
    real_part = 0.0
    imag_part = 0.0
    for column in range(3):
        link_re = link[0][:, column][None]
        link_im = link[1][:, column][None]
        field_re = field[0][:, column:column + 1]
        field_im = field[1][:, column:column + 1]
        real_part = real_part + link_re * field_re - link_im * field_im
        imag_part = imag_part + link_re * field_im + link_im * field_re
    return jnp.stack([real_part, imag_part])


def colour_dagger(link, field):
    real_part = 0.0
    imag_part = 0.0
    for column in range(3):
        link_re = link[0][column][None]
        link_im = link[1][column][None]
        field_re = field[0][:, column:column + 1]
        field_im = field[1][:, column:column + 1]
        real_part = real_part + link_re * field_re + link_im * field_im
        imag_part = imag_part + link_re * field_im - link_im * field_re
    return jnp.stack([real_part, imag_part])


def clover_times(clover, field):
    halves = []
    for chirality in range(2):
        chiral_part = field[:, 2 * chirality:2 * chirality + 2]
        chiral_part = chiral_part.reshape((2, 6) + chiral_part.shape[3:])
        matrix_re = clover[chirality, 0]
        matrix_im = clover[chirality, 1]
        real_part = 0.0
        imag_part = 0.0
        for column in range(6):
            real_part = real_part + matrix_re[:, column] * chiral_part[0, column][None] - matrix_im[:, column] * chiral_part[1, column][None]
            imag_part = imag_part + matrix_re[:, column] * chiral_part[1, column][None] + matrix_im[:, column] * chiral_part[0, column][None]
        halves.append(jnp.stack([real_part, imag_part]).reshape((2, 2, 3) + chiral_part.shape[2:]))
    return jnp.concatenate(halves, axis=1)


def along_y(field, forward):
    column_y = jnp.arange(field.shape[-1], dtype=jnp.int32) % LY
    if forward:
        return jnp.where(column_y == LY - 1, jnp.roll(field, LY - 1, axis=-1), jnp.roll(field, -1, axis=-1))
    return jnp.where(column_y == 0, jnp.roll(field, 1 - LY, axis=-1), jnp.roll(field, 1, axis=-1))


def neighbour(field, direction, forward):
    offset = -1 if forward else 1
    if direction == 0:
        return jnp.roll(field, offset, axis=-3)
    if direction == 1:
        return jnp.roll(field, offset, axis=-2)
    if direction == 2:
        return jnp.roll(field, offset * LY, axis=-1)
    return along_y(field, forward)


def edge_factors(bc_sign, shape):
    count_t, count_z, count_xy = shape
    flat_index = jnp.arange(count_xy, dtype=jnp.int32)
    places = [(jnp.arange(count_t, dtype=jnp.int32)[:, None, None], count_t),
              (jnp.arange(count_z, dtype=jnp.int32)[None, :, None], count_z),
              ((flat_index // LY)[None, None, :], count_xy // LY),
              ((flat_index % LY)[None, None, :], LY)]
    factors = []
    for direction in range(4):
        where_now, extent = places[direction]
        flipped = bc_sign[direction].astype(jnp.float32)
        factors.append((jnp.where(where_now == extent - 1, flipped, 1.0), jnp.where(where_now == 0, flipped, 1.0)))
    return factors


def fine_apply(field, gauge_links, clover, factors):
    result = MASS_TERM * field + clover_times(clover, field)
    for direction in range(4):
        minus_tables = spin_tables(direction, -1)
        plus_tables = spin_tables(direction, 1)
        ahead = colour_times(gauge_links[direction], neighbour(field, direction, True) * factors[direction][0])
        behind = colour_dagger(neighbour(gauge_links[direction], direction, False), neighbour(field, direction, False) * factors[direction][1])
        result = result - 0.5 * (spin_times(minus_tables[0], minus_tables[1], ahead) + spin_times(plus_tables[0], plus_tables[1], behind))
    return result


def source_index(block_slot):
    dev_t, dev_z, dev_x = LT // BLK, LZ // BLK, LX // BLK
    count_t, count_z, count_x = block_slot.shape
    base_t = jnp.arange(count_t, dtype=jnp.int32)[:, None, None] // dev_t * dev_t
    base_z = jnp.arange(count_z, dtype=jnp.int32)[None, :, None] // dev_z * dev_z
    base_x = jnp.arange(count_x, dtype=jnp.int32)[None, None, :] // dev_x * dev_x
    slot_t = block_slot // (dev_z * dev_x)
    slot_z = block_slot // dev_x % dev_z
    slot_x = block_slot % dev_x
    return (((base_t + slot_t) * count_z + base_z + slot_z) * count_x + base_x + slot_x).astype(jnp.int32)


def column_layout(field):
    width = BLK * LY
    shaped = field.reshape((2, 12, CT, BLK, CZ, BLK, CX, width))
    return jnp.moveaxis(shaped, 2, 0)


def restrict_all(rounded, null_store, indices):
    columns = column_layout(rounded)
    flat_store = null_store.reshape((-1,) + null_store.shape[3:])

    def one_slice(inputs):
        field_part, index_part = inputs
        null_rows = jnp.take(flat_store, index_part.reshape(-1), axis=0).astype(jnp.float32)
        null_rows = null_rows.reshape((CZ, CX) + null_rows.shape[1:])
        field_part = field_part.astype(jnp.float32)
        turned = jnp.stack([field_part[1], -field_part[0]])
        paired = jnp.stack([field_part, turned])
        return jnp.einsum('zxpvsabw,qpsazbxw->qvzxw', null_rows, paired, precision=HIGHEST)

    coarse = lax.map(one_slice, (columns, indices))
    coarse = coarse.reshape(coarse.shape[:5] + (BLK, CY, BLK)).sum(axis=(5, 7))
    return jnp.transpose(coarse, (1, 2, 0, 3, 4, 5))


def prolong_all(coarse_round, null_store, indices):
    width = BLK * LY
    per_slice = jnp.moveaxis(coarse_round, 2, 0)
    flat_store = null_store.reshape((-1,) + null_store.shape[3:])

    def one_slice(inputs):
        coarse_part, index_part = inputs
        null_rows = jnp.take(flat_store, index_part.reshape(-1), axis=0).astype(jnp.float32)
        null_rows = null_rows.reshape((CZ, CX) + null_rows.shape[1:])
        coarse_part = coarse_part.astype(jnp.float32)
        spread = jnp.broadcast_to(coarse_part[..., None, :, None], coarse_part.shape[:4] + (BLK, CY, BLK))
        spread = spread.reshape(coarse_part.shape[:4] + (width,))
        mixture = jnp.stack([jnp.stack([spread[0], -spread[1]]), jnp.stack([spread[1], spread[0]])])
        return jnp.einsum('zxpvsabw,qpvzxw->qsazbxw', null_rows, mixture, precision=HIGHEST)

    fine = lax.map(one_slice, (per_slice, indices))
    fine = jnp.moveaxis(fine, 0, 2)
    return fine.reshape((2, 4, 3, CT * BLK, CZ * BLK, CX * width))


def block_times(block_links, stacked):
    links_re = block_links[:, 0]
    links_im = block_links[:, 1]
    vector_re = stacked[:, 0]
    vector_im = stacked[:, 1]
    real_part = jnp.einsum('kijabcd,kjabcd->iabcd', links_re, vector_re, precision=HIGHEST) - jnp.einsum('kijabcd,kjabcd->iabcd', links_im, vector_im, precision=HIGHEST)
    imag_part = jnp.einsum('kijabcd,kjabcd->iabcd', links_re, vector_im, precision=HIGHEST) + jnp.einsum('kijabcd,kjabcd->iabcd', links_im, vector_re, precision=HIGHEST)
    return jnp.stack([real_part, imag_part])


def coarse_apply(vector, coarse_links):
    neighbours = [vector,
                  jnp.roll(vector, -1, 2), jnp.roll(vector, 1, 2),
                  jnp.roll(vector, -1, 3), jnp.roll(vector, 1, 3),
                  jnp.roll(vector, -1, 4), jnp.roll(vector, 1, 4),
                  jnp.roll(vector, -1, 5), jnp.roll(vector, 1, 5)]
    return 2.0 * vector + block_times(coarse_links, jnp.stack(neighbours))


def reference(source, iterate, gauge_links, clover, bc_sign, null_store, block_slot, coarse_links):
    factors = edge_factors(bc_sign, source.shape[3:])
    residual_start = source - fine_apply(iterate, gauge_links, clover, factors)
    indices = source_index(block_slot)
    coarse_rhs = restrict_all(residual_start.astype(jnp.bfloat16), null_store, indices)
    coarse_sol = RELAX_WEIGHT * coarse_rhs
    for iteration in range(CITERS - 1):
        coarse_sol = coarse_sol + RELAX_WEIGHT * (coarse_rhs - coarse_apply(coarse_sol, coarse_links))
    correction = prolong_all(coarse_sol.astype(jnp.bfloat16), null_store, indices)
    new_iterate = iterate + correction
    new_residual = residual_start - fine_apply(correction, gauge_links, clover, factors)
    return new_iterate, new_residual
```

```python
import functools

import jax
import jax.numpy as jnp
from jax import lax
from jax.experimental import pallas as pl
from jax.experimental.pallas import tpu as pltpu
from jax.sharding import PartitionSpec as P

BLK = 4
LY = 32
CITERS = 4
MASS_TERM = 3.8
RELAX_WEIGHT = 0.4
HIGHEST = lax.Precision.HIGHEST
MESH = pl.DeviceIdType.MESH
LANES = 32
F32 = jnp.float32

UPPER = [((0, 0), (1, 0)), ((0, 3), (1, 1)), ((1, 3), (0, 3)), ((1, 2), (0, 0))]
LOWER = [((0, 0), (1, 0)), ((0, 1), (1, 3)), ((1, 1), (0, 1)), ((1, 0), (0, 2))]


def add_turned(a, b, power):
    power %= 4
    if power == 0:
        return (a[0] + b[0], a[1] + b[1])
    if power == 1:
        return (a[0] - b[1], a[1] + b[0])
    if power == 2:
        return (a[0] - b[0], a[1] - b[1])
    return (a[0] + b[1], a[1] - b[0])


def project(psi, mu, forward):
    turn = 2 if forward else 0
    return [
        [add_turned(psi[row][c], psi[2 + UPPER[mu][row][0]][c], UPPER[mu][row][1] + turn) for c in range(3)]
        for row in range(2)
    ]


def rebuild(total, half, mu, forward):
    turn = 2 if forward else 0
    for row in range(2):
        index, power = LOWER[mu][row]
        for c in range(3):
            total[row][c] = add_turned(total[row][c], half[row][c], 0)
            total[2 + row][c] = add_turned(total[2 + row][c], half[index][c], power + turn)


def link_times(link, half):
    out = [[None] * 3 for _ in range(2)]
    for a in range(3):
        for b in range(3):
            ur, ui = link(0, a * 3 + b), link(1, a * 3 + b)
            for s in range(2):
                hr, hi = half[s][b]
                term = (ur * hr - ui * hi, ur * hi + ui * hr)
                out[s][a] = term if b == 0 else add_turned(out[s][a], term, 0)
    return out


def link_dagger(link, half):
    out = [[None] * 3 for _ in range(2)]
    for a in range(3):
        for b in range(3):
            ur, ui = link(0, b * 3 + a), link(1, b * 3 + a)
            for s in range(2):
                hr, hi = half[s][b]
                term = (ur * hr + ui * hi, ur * hi - ui * hr)
                out[s][a] = term if b == 0 else add_turned(out[s][a], term, 0)
    return out


def rows(ref, index, height=8):
    start = index * height
    return ref[pl.ds(start if isinstance(index, int) else pl.multiple_of(start, height), height), :]


def put_rows(ref, index, value, height=8):
    start = index * height
    ref[pl.ds(start if isinstance(index, int) else pl.multiple_of(start, height), height), :] = value


def spinor_of(get):
    return [[(get(s * 3 + c), get(12 + s * 3 + c)) for c in range(3)] for s in range(4)]


def half_of(get):
    return [[(get(s * 3 + c), get(6 + s * 3 + c)) for c in range(3)] for s in range(2)]


def put_half(half, put):
    for s in range(2):
        for c in range(3):
            put(s * 3 + c, half[s][c][0])
            put(6 + s * 3 + c, half[s][c][1])


def map_half(half, change):
    return [[(change(z[0]), change(z[1])) for z in row] for row in half]


def zero_spinor(like):
    return [[(jnp.zeros_like(like), jnp.zeros_like(like)) for _ in range(3)] for _ in range(4)]


def roll(value, shift, axis):
    shift %= value.shape[axis]
    return value if shift == 0 else pltpu.roll(value, shift, axis)


def split_columns(a, b, top):
    return (
        jnp.where(top, a, pltpu.roll(b, BLK, 0)),
        jnp.where(top, pltpu.roll(a, BLK, 0), b),
    )


def wide(a, b):
    return a.astype(F32) * b.astype(F32)


def kernel(
    counts, bc_hbm, slot_hbm, src_hbm, it_hbm, ga_hbm, cl_hbm, nu_hbm, co_hbm, out_it, out_res,
    bc_ref, slot_ref, src, itv, ga, cl, nu, co, res, corr, gx, st, sx, sz, rt, rx, rz, hx, fc, red, pk, part, wbuf,
    wr, rhs, wexp, wv, pc, load_sem, send_sem, recv_sem,
):
    T = BLK
    names = ("ta", "gz", "xy")
    nv = nu.shape[2]

    def load(number, source, target):
        copy = pltpu.make_async_copy(source, target, load_sem.at[number])
        copy.start()
        return copy

    def link_part(ref, mu):
        size = ref.shape[0] // 4
        return ref.at[pl.ds(mu * size, size), :]

    load_it = load(0, it_hbm, itv)
    load_x = load(1, link_part(ga_hbm, 2), link_part(ga, 2))
    place = {n: lax.axis_index(n) for n in names}
    ahead = {n: {n: lax.rem(place[n] + 1, counts[n])} for n in names}
    behind = {n: {n: lax.rem(place[n] + counts[n] - 1, counts[n])} for n in names}
    barrier = pltpu.get_barrier_semaphore()
    for n in ("xy", "ta", "gz"):
        for target in (ahead[n], behind[n]):
            pl.semaphore_signal(barrier, inc=1, device_id=target, device_id_type=MESH)
    load_t = load(2, link_part(ga_hbm, 0), link_part(ga, 0))
    load_z = load(3, link_part(ga_hbm, 1), link_part(ga, 1))
    load_bc = load(4, bc_hbm, bc_ref)
    load_slot = load(5, slot_hbm, slot_ref)
    load_y = load(6, link_part(ga_hbm, 3), link_part(ga, 3))
    load_src = load(7, src_hbm, src)
    load_cl = load(8, cl_hbm, cl)
    load_co = load(9, co_hbm, co)
    load_nu = load(10, nu_hbm, nu)

    def send(phase, number, source, target, device):
        slot = (phase % 2) * 6 + number
        copy = pltpu.make_async_remote_copy(
            src_ref=source, dst_ref=target, send_sem=send_sem.at[slot], recv_sem=recv_sem.at[slot],
            device_id=device, device_id_type=MESH,
        )
        copy.start()
        return copy

    row = lax.broadcasted_iota(jnp.int32, (8, 128), 0)
    lane = lax.broadcasted_iota(jnp.int32, (8, 128), 1)
    column_y = lane & (LY - 1)
    group = lane // LY
    top = row < BLK

    def gauge(mu, t):
        return lambda ri, m: rows(ga, ((mu * 2 + ri) * 9 + m) * T + t)

    def gauge_edge_z(ri, m):
        return ga[pl.ds((((2 + ri) * 9 + m) * T) * 8 + 7, T, stride=8), :]

    def gauge_edge_x(ri, m):
        return rows(gx, ri * 9 + m)

    def site(field, t):
        return spinor_of(lambda k: rows(field, k * T + t))

    def gathered(values, offset):
        moved = [roll(v, LY * t + offset, 1) for t, v in enumerate(values)]
        value = moved[T - 1]
        for t in range(T - 1):
            value = jnp.where(group == t, moved[t], value)
        return value

    def pack_links(ri, carry):
        for m in range(9):
            base = (((4 + ri) * 9 + m) * T)
            put_rows(gx, ri * 9 + m, gathered([rows(ga, base + t) for t in range(T)], LY))
        return carry

    def send_x(d, field):
        sites = [site(field, t) for t in range(T)]
        first_half = [project(psi, 2, True) for psi in sites]
        last_half = [project(psi, 2, False) for psi in sites]

        def joined(halves, offset):
            return [
                [tuple(gathered([h[s][c][ri] for h in halves], offset) for ri in range(2)) for c in range(3)]
                for s in range(2)
            ]

        put_half(joined(first_half, 0), lambda c, v: put_rows(sx.at[d, 0], c, v))
        copy_0 = send(d * 4, 0, sx.at[d, 0], rx.at[d, 0], behind["xy"])
        put_half(link_dagger(gauge_edge_x, joined(last_half, LY)), lambda c, v: put_rows(sx.at[d, 1], c, v))
        copy_1 = send(d * 4, 1, sx.at[d, 1], rx.at[d, 1], ahead["xy"])
        return [copy_0, copy_1]

    def send_t(d, field):
        put_half(project(site(field, 0), 0, True), lambda c, v: put_rows(st.at[d, 0], c, v))
        copy_0 = send(d * 4, 2, st.at[d, 0], rt.at[d, 0], behind["ta"])
        half = link_dagger(gauge(0, T - 1), project(site(field, T - 1), 0, False))
        put_half(half, lambda c, v: put_rows(st.at[d, 1], c, v))
        copy_1 = send(d * 4, 3, st.at[d, 1], rt.at[d, 1], ahead["ta"])
        return [copy_0, copy_1]

    def send_z(d, field):
        low = spinor_of(lambda k: field[pl.ds(k * T * 8, T, stride=8), :])
        put_half(project(low, 1, True), lambda c, v: put_rows(sz.at[d, 0], c, v, T))
        copy_0 = send(d * 4, 4, sz.at[d, 0], rz.at[d, 0], behind["gz"])
        high = spinor_of(lambda k: field[pl.ds(k * T * 8 + 7, T, stride=8), :])
        half = link_dagger(gauge_edge_z, project(high, 1, False))
        put_half(half, lambda c, v: put_rows(sz.at[d, 1], c, v, T))
        copy_1 = send(d * 4, 5, sz.at[d, 1], rz.at[d, 1], ahead["gz"])
        return [copy_0, copy_1]

    def local_part(field, base, out, sign_y):
        def body(t, carry):
            psi = site(field, t)
            total = zero_spinor(psi[0][0][0])

            def up(v):
                return jnp.where(column_y == LY - 1, roll(v, LY - 1, 1) * sign_y, roll(v, -1, 1))

            def down(v):
                return jnp.where(column_y == 0, roll(v, 1 - LY, 1) * sign_y, roll(v, 1, 1))

            rebuild(total, link_times(gauge(3, t), map_half(project(psi, 3, True), up)), 3, True)
            rebuild(total, map_half(link_dagger(gauge(3, t), project(psi, 3, False)), down), 3, False)
            inner = map_half(project(psi, 2, True), lambda v: jnp.where(lane >= 128 - LY, 0.0, roll(v, -LY, 1)))
            rebuild(total, link_times(gauge(2, t), inner), 2, True)
            inner = link_dagger(gauge(2, t), project(psi, 2, False))
            rebuild(total, map_half(inner, lambda v: jnp.where(lane < LY, 0.0, roll(v, LY, 1))), 2, False)
            inner = map_half(project(psi, 1, True), lambda v: jnp.where(row == 7, 0.0, roll(v, -1, 0)))
            rebuild(total, link_times(gauge(1, t), inner), 1, True)
            inner = link_dagger(gauge(1, t), project(psi, 1, False))
            rebuild(total, map_half(inner, lambda v: jnp.where(row == 0, 0.0, roll(v, 1, 0))), 1, False)
            next_t, last_t = lax.rem(t + 1, T), lax.rem(t + T - 1, T)
            inside = jnp.where(t == T - 1, 0.0, 1.0)
            inner = link_times(gauge(0, t), project(site(field, next_t), 0, True))
            rebuild(total, map_half(inner, lambda v: v * inside), 0, True)
            within = jnp.where(t == 0, 0.0, 1.0)
            inner = link_dagger(gauge(0, last_t), project(site(field, last_t), 0, False))
            rebuild(total, map_half(inner, lambda v: v * within), 0, False)
            for ch in range(2):
                for i in range(6):
                    s, c = 2 * ch + i // 3, i % 3
                    re, im = psi[s][c][0] * MASS_TERM, psi[s][c][1] * MASS_TERM
                    for j in range(6):
                        vr, vi = psi[2 * ch + j // 3][j % 3]
                        index = (ch * 2 * 36 + i * 6 + j) * T + t
                        mr, mi = rows(cl, index), rows(cl, index + 36 * T)
                        re = re + (mr * vr - mi * vi)
                        im = im + (mr * vi + mi * vr)
                    k = s * 3 + c
                    here, there = k * T + t, (12 + k) * T + t
                    put_rows(out, here, rows(base, here) - re + 0.5 * total[s][c][0])
                    put_rows(out, there, rows(base, there) - im + 0.5 * total[s][c][1])
            return carry

        lax.fori_loop(0, T, body, 0)

    def add_to(out, total, where):
        for s in range(4):
            for c in range(3):
                for ri in range(2):
                    spot = where(ri * 12 + s * 3 + c)
                    out[spot] = out[spot] + 0.5 * total[s][c][ri]

    def far_part(d, out, copies, last, first):
        copies[4].wait()
        copies[5].wait()
        edge = half_of(lambda c: rows(rz.at[d, 0], c, T) * last[1])
        total = zero_spinor(edge[0][0][0])
        rebuild(total, link_times(gauge_edge_z, edge), 1, True)
        add_to(out, total, lambda k: (pl.ds(k * T * 8 + 7, T, stride=8), slice(None)))
        total = zero_spinor(edge[0][0][0])
        rebuild(total, half_of(lambda c: rows(rz.at[d, 1], c, T) * first[1]), 1, False)
        add_to(out, total, lambda k: (pl.ds(k * T * 8, T, stride=8), slice(None)))
        copies[2].wait()
        copies[3].wait()
        total = zero_spinor(lane.astype(F32))
        edge = half_of(lambda c: rows(rt.at[d, 0], c) * last[0])
        rebuild(total, link_times(gauge(0, T - 1), edge), 0, True)
        add_to(out, total, lambda k: (pl.ds((k * T + T - 1) * 8, 8), slice(None)))
        total = zero_spinor(lane.astype(F32))
        rebuild(total, half_of(lambda c: rows(rt.at[d, 1], c) * first[0]), 0, False)
        add_to(out, total, lambda k: (pl.ds(k * T * 8, 8), slice(None)))
        copies[1].wait()
        copies[0].wait()
        edge = half_of(lambda c: rows(rx.at[d, 0], c) * last[2])
        put_half(link_times(gauge_edge_x, edge), lambda c, v: put_rows(hx, c, v))
        way = jnp.where(group == T - 1, -1.0, 1.0)
        for t in range(T):
            def both(c):
                fore = roll(rows(hx, c), -LY * (t + 1), 1)
                back = roll(rows(rx.at[d, 1], c) * first[2], -LY * t, 1)
                return jnp.where(group == T - 1, fore, jnp.where(group == 0, back, 0.0))

            half = half_of(both)
            total = zero_spinor(lane.astype(F32))
            for s in range(2):
                index, power = LOWER[2][s]
                for c in range(3):
                    total[s][c] = half[s][c]
                    z = half[index][c]
                    total[2 + s][c] = add_turned(total[2 + s][c], (z[0] * way, z[1] * way), power)
            add_to(out, total, lambda k: (pl.ds((k * T + t) * 8, 8), slice(None)))

    load_x.wait()
    lax.fori_loop(0, 2, pack_links, 0)
    load_it.wait()
    pl.semaphore_wait(barrier, 6)
    copies = send_x(0, itv)
    load_t.wait()
    copies += send_t(0, itv)
    load_z.wait()
    copies += send_z(0, itv)
    load_bc.wait()
    load_slot.wait()
    sign = [bc_ref[mu].astype(F32) for mu in range(4)]
    last = [jnp.where(place[n] == counts[n] - 1, sign[i], 1.0) for i, n in enumerate(names)]
    first = [jnp.where(place[n] == 0, sign[i], 1.0) for i, n in enumerate(names)]
    swap = jnp.full((8, 128), slot_ref[0], jnp.int32) != 0
    load_y.wait()
    load_src.wait()
    load_cl.wait()
    local_part(itv, src, res, sign[3])
    load_co.wait()

    def pack_coarse(i, carry):
        for k in range(9):
            parts = []
            for col in range(2):
                for ri in range(2):
                    parts.append(jnp.concatenate([co[k, ri, i, col], jnp.zeros((8, 128 - nv), F32)], axis=1))
            value = parts[0]
            for g in range(1, 4):
                value = jnp.where(group == g, roll(parts[g], LANES * g, 1), value)
            pk[k, i] = value
        return carry

    lax.fori_loop(0, nv, pack_coarse, 0)
    far_part(0, res, copies, last, first)

    def to_columns(k, carry):
        low, high = [], []
        for pair, group_of in enumerate((low, high)):
            a, b = rows(res, k * T + 2 * pair), rows(res, k * T + 2 * pair + 1)
            col_0, col_1 = split_columns(a, b, top)
            group_of.append(jnp.where(swap, col_1, col_0))
            group_of.append(jnp.where(swap, col_0, col_1))
        for slot in range(2):
            value = jnp.concatenate([low[slot], high[slot]], axis=0).astype(jnp.bfloat16)
            fc[slot, k] = value
            fc[slot, 24 + k] = -value
        return carry

    lax.fori_loop(0, 24, to_columns, 0)
    load_nu.wait()
    red[...] = jnp.zeros(red.shape, F32)
    for slot in range(2):
        def restrict(g, carry):
            sums = [None] * 4
            for s in range(12):
                fr, fi, minus = fc[slot, s], fc[slot, 12 + s], fc[slot, 24 + s]
                for j in range(2):
                    nr, ni = nu[slot, 0, g * 2 + j, s], nu[slot, 1, g * 2 + j, s]
                    for q, pair in enumerate(((fr, fi), (fi, minus))):
                        at = 2 * j + q
                        term = wide(nr, pair[0])
                        sums[at] = term if sums[at] is None else sums[at] + term
                        sums[at] = sums[at] + wide(ni, pair[1])
            for j in range(2):
                for ri in range(2):
                    value = sums[2 * j + ri]
                    put_rows(red, (2 * slot + ri) * LANES + g * 2 + j, value[:8] + value[8:])
            return carry

        lax.fori_loop(0, nv // 2, restrict, 0)
    chooser = ((column_y // BLK) == row).astype(F32)
    gathered_rows = red[pl.ds(0, 128, stride=8), :]
    for r in range(1, 8):
        gathered_rows = gathered_rows + red[pl.ds(r, 128, stride=8), :]
    value = lax.dot_general(
        chooser, gathered_rows, (((1,), (1,)), ((), ())), precision=HIGHEST, preferred_element_type=F32
    )
    value = jnp.where(swap, roll(value, 2 * LANES, 1), value)
    rhs[...] = value
    wbuf[0] = RELAX_WEIGHT * value

    even = (group & 1) == 0
    turn = jnp.where(even, 1.0, -1.0)

    def pairs_of(w):
        return w * turn, jnp.where(even, roll(w, -LANES, 1), roll(w, LANES, 1))

    def products(vectors, i, sums):
        for k, (wa, wb) in vectors:
            y = pk[k, i]
            sums = (y * wa, y * wb) if sums is None else (sums[0] + y * wa, sums[1] + y * wb)
        return sums

    block = 8
    for it in range(CITERS - 1):
        phase = it + 1
        own = wbuf[it]
        targets = [behind["xy"], ahead["xy"], behind["ta"], ahead["ta"], behind["gz"], ahead["gz"]]
        copies = [send(phase, d, wbuf.at[it], wr.at[it, d], targets[d]) for d in range(6)]
        vectors = [(0, pairs_of(own)), (7, pairs_of(roll(own, -1, 0))), (8, pairs_of(roll(own, 1, 0)))]

        def near(g, carry):
            for j in range(block):
                i = g * block + j
                part[0, i], part[1, i] = products(vectors, i, None)
            return carry

        lax.fori_loop(0, nv // block, near, 0)
        copies[4].wait()
        copies[5].wait()
        half = 2 * LANES
        next_z = jnp.where(lane < half, roll(own, half, 1), roll(wr[it, 4], half, 1))
        last_z = jnp.where(lane < half, roll(wr[it, 5], half, 1), roll(own, half, 1))
        z_vectors = [(3, pairs_of(next_z)), (4, pairs_of(last_z))]

        def middle(g, carry):
            for j in range(block):
                i = g * block + j
                part[0, i], part[1, i] = products(z_vectors, i, (part[0, i], part[1, i]))
            return carry

        lax.fori_loop(0, nv // block, middle, 0)
        for d in range(4):
            copies[d].wait()
        far_vectors = [(k, pairs_of(wr[it, d])) for k, d in ((1, 2), (2, 3), (5, 0), (6, 1))]
        applied = jnp.zeros((8, 128), F32)
        for i in range(nv):
            sums = products(far_vectors, i, (part[0, i], part[1, i]))
            for ri in range(2):
                for col in range(2):
                    mine = (lane < half) if col == 0 else (lane >= half)
                    whole = jnp.sum(jnp.where(mine, sums[ri], 0.0), axis=1, keepdims=True)
                    applied = jnp.where(lane == LANES * (2 * col + ri) + i, whole, applied)
        wbuf[it + 1] = own + RELAX_WEIGHT * (rhs[...] - (2.0 * own + applied))

    w = wbuf[CITERS - 1]
    w = jnp.where(swap, roll(w, 2 * LANES, 1), w).astype(jnp.bfloat16)
    wexp[...] = lax.dot_general(
        w, chooser.astype(jnp.bfloat16), (((0,), (0,)), ((), ())), preferred_element_type=F32
    )

    def spread(c, carry):
        for slot in range(2):
            values = [wexp[pl.ds((2 * slot + ri) * LANES + c, 1), :] for ri in range(2)]
            for at, v in enumerate((values[0], values[1], -values[1])):
                wv[slot, at, c] = jnp.broadcast_to(v, (2 * 8, 128)).astype(jnp.bfloat16)
        return carry

    lax.fori_loop(0, nv, spread, 0)
    for slot in range(2):
        def prolong(q, carry):
            sums = [None] * 4
            for c in range(nv):
                vr, vi, minus = wv[slot, 0, c], wv[slot, 1, c], wv[slot, 2, c]
                for j in range(2):
                    nr, ni = nu[slot, 0, c, q * 2 + j], nu[slot, 1, c, q * 2 + j]
                    for ri, pair in enumerate(((vr, minus), (vi, vr))):
                        at = 2 * j + ri
                        term = wide(nr, pair[0])
                        sums[at] = term if sums[at] is None else sums[at] + term
                        sums[at] = sums[at] + wide(ni, pair[1])
            for j in range(2):
                for ri in range(2):
                    pc[slot, ri * 12 + q * 2 + j] = sums[2 * j + ri]
            return carry

        lax.fori_loop(0, 6, prolong, 0)

    def from_columns(k, carry):
        for pair in range(2):
            part_0, part_1 = pc[0, k, pl.ds(8 * pair, 8), :], pc[1, k, pl.ds(8 * pair, 8), :]
            part_0, part_1 = jnp.where(swap, part_1, part_0), jnp.where(swap, part_0, part_1)
            for h, value in enumerate(split_columns(part_0, part_1, top)):
                at = k * T + 2 * pair + h
                put_rows(corr, at, value)
                put_rows(out_it, at, rows(itv, at) + value)
        return carry

    lax.fori_loop(0, 24, from_columns, 0)
    copies = send_x(1, corr) + send_t(1, corr) + send_z(1, corr)
    local_part(corr, res, out_res, sign[3])
    far_part(1, out_res, copies, last, first)


def hand_over(it_in, res_in, it_out, res_out, sem):
    copies = [
        pltpu.make_async_copy(a, b, sem.at[i]) for i, (a, b) in enumerate(((it_in, it_out), (res_in, res_out)))
    ]
    for copy in copies:
        copy.start()
    for copy in copies:
        copy.wait()


def per_device(counts, source, iterate, gauge_links, clover, bc_sign, null_store, block_slot, coarse_links):
    lattice = source.shape[3:]
    T = lattice[0]
    columns = block_slot.size
    nv = null_store.shape[4]
    assert lattice == (BLK, 2 * BLK, BLK * LY) and columns == 2 and nv % 8 == 0 and nv <= LANES
    nulls = (columns,) + null_store.shape[3:6] + (BLK * BLK, BLK * LY)
    links = jnp.transpose(coarse_links, (0, 1, 2, 4, 5, 6, 7, 3))
    links = links.reshape(links.shape[:3] + (columns,) + links.shape[6:])
    tall = T * lattice[1]
    field = (24 * tall, lattice[2])
    half = 12 * lattice[1]
    tile = lattice[1:]
    hbm = pl.BlockSpec(memory_space=pltpu.HBM)
    vmem = pl.BlockSpec(memory_space=pltpu.VMEM)
    outs = pl.pallas_call(
        functools.partial(kernel, counts),
        out_shape=(pltpu.VMEM(field, F32),) * 2,
        in_specs=[hbm] * 8,
        out_specs=(vmem,) * 2,
        scratch_shapes=[
            pltpu.SMEM(bc_sign.shape, jnp.int32),
            pltpu.SMEM((columns,), jnp.int32),
            pltpu.VMEM(field, F32),
            pltpu.VMEM(field, F32),
            pltpu.VMEM((72 * tall, 128), F32),
            pltpu.VMEM((144 * tall, 128), F32),
            pltpu.VMEM(nulls, jnp.bfloat16),
            pltpu.VMEM(links.shape, F32),
            pltpu.VMEM(field, F32),
            pltpu.VMEM(field, F32),
            pltpu.VMEM((18 * 8, 128), F32),
            pltpu.VMEM((2, 2, half, 128), F32),
            pltpu.VMEM((2, 2, half, 128), F32),
            pltpu.VMEM((2, 2, 12 * T, 128), F32),
            pltpu.VMEM((2, 2, half, 128), F32),
            pltpu.VMEM((2, 2, half, 128), F32),
            pltpu.VMEM((2, 2, 12 * T, 128), F32),
            pltpu.VMEM((half, 128), F32),
            pltpu.VMEM((columns, 48, BLK * BLK, 128), jnp.bfloat16),
            pltpu.VMEM((128 * 8, 128), F32),
            pltpu.VMEM((9, nv) + tile, F32),
            pltpu.VMEM((2, nv) + tile, F32),
            pltpu.VMEM((CITERS,) + tile, F32),
            pltpu.VMEM((CITERS - 1, 6) + tile, F32),
            pltpu.VMEM(tile, F32),
            pltpu.VMEM((128, 128), F32),
            pltpu.VMEM((columns, 3, nv, BLK * BLK, 128), jnp.bfloat16),
            pltpu.VMEM((columns, 24, BLK * BLK, 128), F32),
            pltpu.SemaphoreType.DMA((11,)),
            pltpu.SemaphoreType.DMA((12,)),
            pltpu.SemaphoreType.DMA((12,)),
        ],
        compiler_params=pltpu.CompilerParams(
            collective_id=0, has_side_effects=True, vmem_limit_bytes=66_200_000
        ),
    )(
        bc_sign,
        block_slot.reshape(-1),
        source.reshape(field),
        iterate.reshape(field),
        gauge_links.reshape(72 * tall, 128),
        clover.reshape(144 * tall, 128),
        null_store.reshape(nulls),
        links,
    )
    outs = pl.pallas_call(
        hand_over,
        out_shape=(jax.ShapeDtypeStruct(field, F32),) * 2,
        in_specs=[pl.BlockSpec(memory_space=pl.ANY)] * 2,
        out_specs=(hbm,) * 2,
        scratch_shapes=[pltpu.SemaphoreType.DMA((2,))],
        compiler_params=pltpu.CompilerParams(vmem_limit_bytes=66_200_000),
    )(*outs)
    return tuple(out.reshape(source.shape) for out in outs)


def solution(mesh):
    placed = (
        P(None, None, None, "ta", "gz", "xy"),
        P(None, None, None, "ta", "gz", "xy"),
        P(None, None, None, None, "ta", "gz", "xy"),
        P(None, None, None, None, "ta", "gz", "xy"),
        P(),
        P("ta", "gz", "xy", None, None, None, None, None, None),
        P("ta", "gz", "xy"),
        P(None, None, None, None, "ta", "gz", "xy", None),
    )
    return jax.shard_map(
        functools.partial(per_device, dict(mesh.shape)),
        mesh=mesh,
        in_specs=placed,
        out_specs=(P(None, None, None, "ta", "gz", "xy"), P(None, None, None, "ta", "gz", "xy")),
        check_vma=False,
    )
```

```python
import functools

import jax
import jax.numpy as jnp
from jax import lax
from jax.experimental import pallas as pl
from jax.experimental.pallas import tpu as pltpu
from jax.sharding import PartitionSpec as P

BLK = 4
LY = 32
CITERS = 4
MASS_TERM = 3.8
RELAX_WEIGHT = 0.4
MESH = pl.DeviceIdType.MESH
LANES = 32
F32 = jnp.float32

UPPER = [((0, 0), (1, 0)), ((0, 3), (1, 1)), ((1, 3), (0, 3)), ((1, 2), (0, 0))]
LOWER = [((0, 0), (1, 0)), ((0, 1), (1, 3)), ((1, 1), (0, 1)), ((1, 0), (0, 2))]


def add_turned(a, b, power):
    power %= 4
    if power == 0:
        return (a[0] + b[0], a[1] + b[1])
    if power == 1:
        return (a[0] - b[1], a[1] + b[0])
    if power == 2:
        return (a[0] - b[0], a[1] - b[1])
    return (a[0] + b[1], a[1] - b[0])


def project(psi, mu, forward):
    turn = 2 if forward else 0
    return [
        [add_turned(psi[row][c], psi[2 + UPPER[mu][row][0]][c], UPPER[mu][row][1] + turn) for c in range(3)]
        for row in range(2)
    ]


def rebuild(total, half, mu, forward):
    turn = 2 if forward else 0
    for row in range(2):
        index, power = LOWER[mu][row]
        for c in range(3):
            total[row][c] = add_turned(total[row][c], half[row][c], 0)
            total[2 + row][c] = add_turned(total[2 + row][c], half[index][c], power + turn)


def link_times(link, half):
    out = [[None] * 3 for _ in range(2)]
    for a in range(3):
        for b in range(3):
            ur, ui = link(0, a * 3 + b), link(1, a * 3 + b)
            for s in range(2):
                hr, hi = half[s][b]
                term = (ur * hr - ui * hi, ur * hi + ui * hr)
                out[s][a] = term if b == 0 else add_turned(out[s][a], term, 0)
    return out


def link_dagger(link, half):
    out = [[None] * 3 for _ in range(2)]
    for a in range(3):
        for b in range(3):
            ur, ui = link(0, b * 3 + a), link(1, b * 3 + a)
            for s in range(2):
                hr, hi = half[s][b]
                term = (ur * hr + ui * hi, ur * hi - ui * hr)
                out[s][a] = term if b == 0 else add_turned(out[s][a], term, 0)
    return out


def rows(ref, index, height=8):
    start = index * height
    return ref[pl.ds(start if isinstance(index, int) else pl.multiple_of(start, height), height), :]


def put_rows(ref, index, value, height=8):
    start = index * height
    ref[pl.ds(start if isinstance(index, int) else pl.multiple_of(start, height), height), :] = value


def spinor_of(get):
    return [[(get(s * 3 + c), get(12 + s * 3 + c)) for c in range(3)] for s in range(4)]


def half_of(get):
    return [[(get(s * 3 + c), get(6 + s * 3 + c)) for c in range(3)] for s in range(2)]


def put_half(half, put):
    for s in range(2):
        for c in range(3):
            put(s * 3 + c, half[s][c][0])
            put(6 + s * 3 + c, half[s][c][1])


def map_half(half, change):
    return [[(change(z[0]), change(z[1])) for z in row] for row in half]


def zero_spinor(like):
    return [[(jnp.zeros_like(like), jnp.zeros_like(like)) for _ in range(3)] for _ in range(4)]


def roll(value, shift, axis):
    shift %= value.shape[axis]
    return value if shift == 0 else pltpu.roll(value, shift, axis)


def split_columns(a, b, top):
    return (
        jnp.where(top, a, pltpu.roll(b, BLK, 0)),
        jnp.where(top, pltpu.roll(a, BLK, 0), b),
    )


def wide(a, b):
    return a.astype(F32) * b.astype(F32)


def kernel(
    counts, bc_hbm, slot_hbm, src_hbm, it_hbm, ga_hbm, cl_hbm, nu_hbm, co_hbm, out_it, out_res,
    bc_ref, slot_ref, src, itv, ga, cl, nu, co, res, corr, gx, st, sx, sz, rt, rx, rz, hx, fc, red, pk, part, wbuf,
    wr, rhs, wexp, wv, pc, load_sem, send_sem, recv_sem,
):
    T = BLK
    names = ("ta", "gz", "xy")
    nv = nu.shape[2]

    def load(number, source, target):
        copy = pltpu.make_async_copy(source, target, load_sem.at[number])
        copy.start()
        return copy

    def link_part(ref, mu):
        size = ref.shape[0] // 4
        return ref.at[pl.ds(mu * size, size), :]

    load_it = load(0, it_hbm, itv)
    load_x = load(1, link_part(ga_hbm, 2), link_part(ga, 2))
    place = {n: lax.axis_index(n) for n in names}
    ahead = {n: {n: lax.rem(place[n] + 1, counts[n])} for n in names}
    behind = {n: {n: lax.rem(place[n] + counts[n] - 1, counts[n])} for n in names}
    barrier = pltpu.get_barrier_semaphore()
    for n in ("xy", "ta", "gz"):
        for target in (ahead[n], behind[n]):
            pl.semaphore_signal(barrier, inc=1, device_id=target, device_id_type=MESH)
    load_t = load(2, link_part(ga_hbm, 0), link_part(ga, 0))
    load_z = load(3, link_part(ga_hbm, 1), link_part(ga, 1))
    load_bc = load(4, bc_hbm, bc_ref)
    load_slot = load(5, slot_hbm, slot_ref)
    load_y = load(6, link_part(ga_hbm, 3), link_part(ga, 3))
    load_src = load(7, src_hbm, src)
    load_cl = load(8, cl_hbm, cl)
    load_co = load(9, co_hbm, co)
    load_nu = load(10, nu_hbm, nu)

    def send(phase, number, source, target, device):
        slot = (phase % 2) * 6 + number
        copy = pltpu.make_async_remote_copy(
            src_ref=source, dst_ref=target, send_sem=send_sem.at[slot], recv_sem=recv_sem.at[slot],
            device_id=device, device_id_type=MESH,
        )
        copy.start()
        return copy

    row = lax.broadcasted_iota(jnp.int32, (8, 128), 0)
    lane = lax.broadcasted_iota(jnp.int32, (8, 128), 1)
    column_y = lane & (LY - 1)
    group = lane // LY
    top = row < BLK

    def gauge(mu, t):
        return lambda ri, m: rows(ga, ((mu * 2 + ri) * 9 + m) * T + t)

    def gauge_edge_z(ri, m):
        return ga[pl.ds((((2 + ri) * 9 + m) * T) * 8 + 7, T, stride=8), :]

    def gauge_edge_x(ri, m):
        return rows(gx, ri * 9 + m)

    def site(field, t):
        return spinor_of(lambda k: rows(field, k * T + t))

    def gathered(values, offset):
        moved = [roll(v, LY * t + offset, 1) for t, v in enumerate(values)]
        value = moved[T - 1]
        for t in range(T - 1):
            value = jnp.where(group == t, moved[t], value)
        return value

    def pack_links(ri, carry):
        for m in range(9):
            base = (((4 + ri) * 9 + m) * T)
            put_rows(gx, ri * 9 + m, gathered([rows(ga, base + t) for t in range(T)], LY))
        return carry

    def ordered(d, number, name, outgoing, incoming, choice):
        copies = [None, None]
        for turn in range(2):
            way = choice if turn == 0 else 1 - choice
            target = {name: lax.rem(place[name] + counts[name] - 1 + 2 * way, counts[name])}
            copies[turn] = send(d * 4, number + way, outgoing.at[d, way], incoming.at[d, way], target)
        return copies

    def fill_x(d, field):
        sites = [site(field, t) for t in range(T)]

        def joined(forward, offset):
            halves = [project(psi, 2, forward) for psi in sites]
            return [
                [tuple(gathered([h[s][c][ri] for h in halves], offset) for ri in range(2)) for c in range(3)]
                for s in range(2)
            ]

        put_half(joined(True, 0), lambda c, v: put_rows(sx.at[d, 0], c, v))
        put_half(link_dagger(gauge_edge_x, joined(False, LY)), lambda c, v: put_rows(sx.at[d, 1], c, v))

    def fill_t(d, field):
        put_half(project(site(field, 0), 0, True), lambda c, v: put_rows(st.at[d, 0], c, v))
        half = link_dagger(gauge(0, T - 1), project(site(field, T - 1), 0, False))
        put_half(half, lambda c, v: put_rows(st.at[d, 1], c, v))

    def fill_z(d, field):
        low = spinor_of(lambda k: field[pl.ds(k * T * 8, T, stride=8), :])
        put_half(project(low, 1, True), lambda c, v: put_rows(sz.at[d, 0], c, v, T))
        high = spinor_of(lambda k: field[pl.ds(k * T * 8 + 7, T, stride=8), :])
        half = link_dagger(gauge_edge_z, project(high, 1, False))
        put_half(half, lambda c, v: put_rows(sz.at[d, 1], c, v, T))

    def send_all(d, field, before):
        before[0]()
        fill_t(d, field)
        copies_t = ordered(d, 2, "ta", st, rt, lax.rem(place["ta"], 2))
        before[1]()
        fill_x(d, field)
        copies_x = ordered(d, 0, "xy", sx, rx, (place["xy"] + 1) // counts["xy"])
        before[2]()
        fill_z(d, field)
        copies_z = ordered(d, 4, "gz", sz, rz, 0)
        return copies_x + copies_t + copies_z

    def local_part(field, base, out, sign_y, before):
        def keep(total, t, old):
            for s in range(4):
                for c in range(3):
                    for ri in range(2):
                        at = (ri * 12 + s * 3 + c) * T + t
                        value = 0.5 * total[s][c][ri]
                        put_rows(out, at, rows(out, at) + value if old else value)

        def inside_tile(t, carry):
            psi = site(field, t)
            total = zero_spinor(psi[0][0][0])
            inner = map_half(project(psi, 2, True), lambda v: jnp.where(lane >= 128 - LY, 0.0, roll(v, -LY, 1)))
            rebuild(total, link_times(gauge(2, t), inner), 2, True)
            inner = link_dagger(gauge(2, t), project(psi, 2, False))
            rebuild(total, map_half(inner, lambda v: jnp.where(lane < LY, 0.0, roll(v, LY, 1))), 2, False)
            inner = map_half(project(psi, 1, True), lambda v: jnp.where(row == 7, 0.0, roll(v, -1, 0)))
            rebuild(total, link_times(gauge(1, t), inner), 1, True)
            inner = link_dagger(gauge(1, t), project(psi, 1, False))
            rebuild(total, map_half(inner, lambda v: jnp.where(row == 0, 0.0, roll(v, 1, 0))), 1, False)
            keep(total, t, False)
            return carry

        lax.fori_loop(0, T, inside_tile, 0)
        before[0]()

        def along_t_y(t, carry):
            total = zero_spinor(lane.astype(F32))
            next_t, last_t = lax.rem(t + 1, T), lax.rem(t + T - 1, T)
            inside = jnp.where(t == T - 1, 0.0, 1.0)
            inner = link_times(gauge(0, t), project(site(field, next_t), 0, True))
            rebuild(total, map_half(inner, lambda v: v * inside), 0, True)
            within = jnp.where(t == 0, 0.0, 1.0)
            inner = link_dagger(gauge(0, last_t), project(site(field, last_t), 0, False))
            rebuild(total, map_half(inner, lambda v: v * within), 0, False)
            psi = site(field, t)

            def up(v):
                return jnp.where(column_y == LY - 1, roll(v, LY - 1, 1) * sign_y, roll(v, -1, 1))

            def down(v):
                return jnp.where(column_y == 0, roll(v, 1 - LY, 1) * sign_y, roll(v, 1, 1))

            rebuild(total, link_times(gauge(3, t), map_half(project(psi, 3, True), up)), 3, True)
            rebuild(total, map_half(link_dagger(gauge(3, t), project(psi, 3, False)), down), 3, False)
            keep(total, t, True)
            return carry

        lax.fori_loop(0, T, along_t_y, 0)
        before[1]()

        def on_site(t, carry):
            psi = site(field, t)
            for ch in range(2):
                for i in range(6):
                    s, c = 2 * ch + i // 3, i % 3
                    re, im = psi[s][c][0] * MASS_TERM, psi[s][c][1] * MASS_TERM
                    for j in range(6):
                        vr, vi = psi[2 * ch + j // 3][j % 3]
                        index = (ch * 2 * 36 + i * 6 + j) * T + t
                        mr, mi = rows(cl, index), rows(cl, index + 36 * T)
                        re = re + (mr * vr - mi * vi)
                        im = im + (mr * vi + mi * vr)
                    k = s * 3 + c
                    here, there = k * T + t, (12 + k) * T + t
                    put_rows(out, here, rows(out, here) + rows(base, here) - re)
                    put_rows(out, there, rows(out, there) + rows(base, there) - im)
            return carry

        lax.fori_loop(0, T, on_site, 0)

    def add_to(out, total, where):
        for s in range(4):
            for c in range(3):
                for ri in range(2):
                    spot = where(ri * 12 + s * 3 + c)
                    out[spot] = out[spot] + 0.5 * total[s][c][ri]

    def far_part(d, out, copies, last, first):
        copies[4].wait()
        copies[5].wait()
        edge = half_of(lambda c: rows(rz.at[d, 0], c, T) * last[1])
        total = zero_spinor(edge[0][0][0])
        rebuild(total, link_times(gauge_edge_z, edge), 1, True)
        add_to(out, total, lambda k: (pl.ds(k * T * 8 + 7, T, stride=8), slice(None)))
        total = zero_spinor(edge[0][0][0])
        rebuild(total, half_of(lambda c: rows(rz.at[d, 1], c, T) * first[1]), 1, False)
        add_to(out, total, lambda k: (pl.ds(k * T * 8, T, stride=8), slice(None)))
        copies[2].wait()
        copies[3].wait()
        total = zero_spinor(lane.astype(F32))
        edge = half_of(lambda c: rows(rt.at[d, 0], c) * last[0])
        rebuild(total, link_times(gauge(0, T - 1), edge), 0, True)
        add_to(out, total, lambda k: (pl.ds((k * T + T - 1) * 8, 8), slice(None)))
        total = zero_spinor(lane.astype(F32))
        rebuild(total, half_of(lambda c: rows(rt.at[d, 1], c) * first[0]), 0, False)
        add_to(out, total, lambda k: (pl.ds(k * T * 8, 8), slice(None)))
        copies[1].wait()
        copies[0].wait()
        edge = half_of(lambda c: rows(rx.at[d, 0], c) * last[2])
        put_half(link_times(gauge_edge_x, edge), lambda c, v: put_rows(hx, c, v))
        way = jnp.where(group == T - 1, -1.0, 1.0)
        for t in range(T):
            def both(c):
                fore = roll(rows(hx, c), -LY * (t + 1), 1)
                back = roll(rows(rx.at[d, 1], c) * first[2], -LY * t, 1)
                return jnp.where(group == T - 1, fore, jnp.where(group == 0, back, 0.0))

            half = half_of(both)
            total = zero_spinor(lane.astype(F32))
            for s in range(2):
                index, power = LOWER[2][s]
                for c in range(3):
                    total[s][c] = half[s][c]
                    z = half[index][c]
                    total[2 + s][c] = add_turned(total[2 + s][c], (z[0] * way, z[1] * way), power)
            add_to(out, total, lambda k: (pl.ds((k * T + t) * 8, 8), slice(None)))

    def ready_t():
        load_it.wait()
        load_t.wait()
        pl.semaphore_wait(barrier, 6)

    def ready_x():
        load_x.wait()
        lax.fori_loop(0, 2, pack_links, 0)

    copies = send_all(0, itv, (ready_t, ready_x, load_z.wait))
    load_bc.wait()
    load_slot.wait()
    sign = [bc_ref[mu].astype(F32) for mu in range(4)]
    last = [jnp.where(place[n] == counts[n] - 1, sign[i], 1.0) for i, n in enumerate(names)]
    first = [jnp.where(place[n] == 0, sign[i], 1.0) for i, n in enumerate(names)]
    swap = jnp.full((8, 128), slot_ref[0], jnp.int32) != 0

    def ready_site():
        load_src.wait()
        load_cl.wait()

    local_part(itv, src, res, sign[3], (load_y.wait, ready_site))

    def pack_coarse(k, carry):
        for i in range(nv):
            parts = [co[k, ri, i, col] for col in range(2) for ri in range(2)]
            parts = [jnp.concatenate([v, jnp.zeros((8, 128 - nv), F32)], axis=1) for v in parts]
            value = parts[0]
            for g in range(1, 4):
                value = value + roll(parts[g], LANES * g, 1)
            pk[k, i] = value
        return carry

    far_part(0, res, copies, last, first)

    def to_columns(k, carry):
        low, high = [], []
        for pair, group_of in enumerate((low, high)):
            a, b = rows(res, k * T + 2 * pair), rows(res, k * T + 2 * pair + 1)
            col_0, col_1 = split_columns(a, b, top)
            group_of.append(jnp.where(swap, col_1, col_0))
            group_of.append(jnp.where(swap, col_0, col_1))
        for slot in range(2):
            value = jnp.concatenate([low[slot], high[slot]], axis=0).astype(jnp.bfloat16)
            fc[slot, k] = value
            fc[slot, 24 + k] = -value
        return carry

    lax.fori_loop(0, 24, to_columns, 0)
    load_nu.wait()
    red[...] = jnp.zeros(red.shape, F32)
    for slot in range(2):
        def restrict(g, carry):
            sums = [None] * 4
            for s in range(12):
                fr, fi, minus = fc[slot, s], fc[slot, 12 + s], fc[slot, 24 + s]
                for j in range(2):
                    nr, ni = nu[slot, 0, g * 2 + j, s], nu[slot, 1, g * 2 + j, s]
                    for q, pair in enumerate(((fr, fi), (fi, minus))):
                        at = 2 * j + q
                        term = wide(nr, pair[0])
                        sums[at] = term if sums[at] is None else sums[at] + term
                        sums[at] = sums[at] + wide(ni, pair[1])
            for j in range(2):
                for ri in range(2):
                    value = sums[2 * j + ri]
                    put_rows(red, (2 * slot + ri) * LANES + g * 2 + j, value[:8] + value[8:])
            return carry

        lax.fori_loop(0, nv // 2, restrict, 0)
    gathered_rows = red[pl.ds(0, 128, stride=8), :]
    for r in range(1, 8):
        gathered_rows = gathered_rows + red[pl.ds(r, 128, stride=8), :]
    turned = jnp.transpose(gathered_rows)
    value = None
    for m in range(4):
        part_sum = turned[8 * m:8 * m + 8]
        for x in range(1, BLK):
            part_sum = part_sum + turned[LY * x + 8 * m:LY * x + 8 * m + 8]
        part_sum = part_sum + roll(part_sum, 1, 0)
        part_sum = part_sum + roll(part_sum, 2, 0)
        lower, upper = roll(part_sum, 2 * m - 3, 0), roll(part_sum, 2 * m + 1 - 7, 0)
        here = jnp.where(row == 2 * m, lower, upper)
        value = here if m == 0 else jnp.where(row // 2 == m, here, value)
    value = jnp.where(swap, roll(value, 2 * LANES, 1), value)
    rhs[...] = value
    wbuf[0] = RELAX_WEIGHT * value

    even = (group & 1) == 0
    turn = jnp.where(even, 1.0, -1.0)

    def pairs_of(w):
        return w * turn, jnp.where(even, roll(w, -LANES, 1), roll(w, LANES, 1))

    def products(vectors, i, sums):
        for k, (wa, wb) in vectors:
            y = pk[k, i]
            sums = (y * wa, y * wb) if sums is None else (sums[0] + y * wa, sums[1] + y * wb)
        return sums

    block = 8
    for it in range(CITERS - 1):
        phase = it + 1
        own = wbuf[it]
        targets = [behind["xy"], ahead["xy"], behind["ta"], ahead["ta"], behind["gz"], ahead["gz"]]
        copies = [send(phase, d, wbuf.at[it], wr.at[it, d], targets[d]) for d in range(6)]
        if it == 0:
            load_co.wait()
            lax.fori_loop(0, 9, pack_coarse, 0)
        vectors = [(0, pairs_of(own)), (7, pairs_of(roll(own, -1, 0))), (8, pairs_of(roll(own, 1, 0)))]

        def near(g, carry):
            for j in range(block):
                i = g * block + j
                part[0, i], part[1, i] = products(vectors, i, None)
            return carry

        lax.fori_loop(0, nv // block, near, 0)
        copies[4].wait()
        copies[5].wait()
        half = 2 * LANES
        next_z = jnp.where(lane < half, roll(own, half, 1), roll(wr[it, 4], half, 1))
        last_z = jnp.where(lane < half, roll(wr[it, 5], half, 1), roll(own, half, 1))
        z_vectors = [(3, pairs_of(next_z)), (4, pairs_of(last_z))]

        def middle(g, carry):
            for j in range(block):
                i = g * block + j
                part[0, i], part[1, i] = products(z_vectors, i, (part[0, i], part[1, i]))
            return carry

        lax.fori_loop(0, nv // block, middle, 0)
        for d in range(4):
            copies[d].wait()
        far_vectors = [(k, pairs_of(wr[it, d])) for k, d in ((1, 2), (2, 3), (5, 0), (6, 1))]
        applied = jnp.zeros((8, 128), F32)
        for i in range(nv):
            sums = products(far_vectors, i, (part[0, i], part[1, i]))
            for ri in range(2):
                for col in range(2):
                    mine = (lane < half) if col == 0 else (lane >= half)
                    whole = jnp.sum(jnp.where(mine, sums[ri], 0.0), axis=1, keepdims=True)
                    applied = jnp.where(lane == LANES * (2 * col + ri) + i, whole, applied)
        wbuf[it + 1] = own + RELAX_WEIGHT * (rhs[...] - (2.0 * own + applied))

    w = wbuf[CITERS - 1]
    w = jnp.where(swap, roll(w, 2 * LANES, 1), w)
    tall = []
    for m in range(4):
        low, high = jnp.broadcast_to(w[2 * m:2 * m + 1], (8, 128)), jnp.broadcast_to(w[2 * m + 1:2 * m + 2], (8, 128))
        tall.append(jnp.where(top, low, high))
    wexp[...] = jnp.transpose(jnp.concatenate(tall * BLK, axis=0))

    def spread(c, carry):
        for slot in range(2):
            values = [wexp[pl.ds((2 * slot + ri) * LANES + c, 1), :] for ri in range(2)]
            for at, v in enumerate((values[0], values[1], -values[1])):
                wv[slot, at, c] = jnp.broadcast_to(v, (2 * 8, 128)).astype(jnp.bfloat16)
        return carry

    lax.fori_loop(0, nv, spread, 0)
    for slot in range(2):
        def prolong(q, carry):
            sums = [None] * 4
            for c in range(nv):
                vr, vi, minus = wv[slot, 0, c], wv[slot, 1, c], wv[slot, 2, c]
                for j in range(2):
                    nr, ni = nu[slot, 0, c, q * 2 + j], nu[slot, 1, c, q * 2 + j]
                    for ri, pair in enumerate(((vr, minus), (vi, vr))):
                        at = 2 * j + ri
                        term = wide(nr, pair[0])
                        sums[at] = term if sums[at] is None else sums[at] + term
                        sums[at] = sums[at] + wide(ni, pair[1])
            for j in range(2):
                for ri in range(2):
                    pc[slot, ri * 12 + q * 2 + j] = sums[2 * j + ri]
            return carry

        lax.fori_loop(0, 6, prolong, 0)

    def from_columns(k, carry):
        for pair in range(2):
            part_0, part_1 = pc[0, k, pl.ds(8 * pair, 8), :], pc[1, k, pl.ds(8 * pair, 8), :]
            part_0, part_1 = jnp.where(swap, part_1, part_0), jnp.where(swap, part_0, part_1)
            for h, value in enumerate(split_columns(part_0, part_1, top)):
                at = k * T + 2 * pair + h
                put_rows(corr, at, value)
                put_rows(out_it, at, rows(itv, at) + value)
        return carry

    lax.fori_loop(0, 24, from_columns, 0)
    nothing = lambda: None
    copies = send_all(1, corr, (nothing,) * 3)
    local_part(corr, res, out_res, sign[3], (nothing,) * 2)
    far_part(1, out_res, copies, last, first)


def hand_over(it_in, res_in, it_out, res_out, sem):
    copies = [
        pltpu.make_async_copy(a, b, sem.at[i]) for i, (a, b) in enumerate(((it_in, it_out), (res_in, res_out)))
    ]
    for copy in copies:
        copy.start()
    for copy in copies:
        copy.wait()


def per_device(counts, source, iterate, gauge_links, clover, bc_sign, null_store, block_slot, coarse_links):
    lattice = source.shape[3:]
    T = lattice[0]
    columns = block_slot.size
    nv = null_store.shape[4]
    assert lattice == (BLK, 2 * BLK, BLK * LY) and columns == 2 and nv % 8 == 0 and nv <= LANES
    nulls = (columns,) + null_store.shape[3:6] + (BLK * BLK, BLK * LY)
    links = jnp.transpose(coarse_links, (0, 1, 2, 4, 5, 6, 7, 3))
    links = links.reshape(links.shape[:3] + (columns,) + links.shape[6:])
    tall = T * lattice[1]
    field = (24 * tall, lattice[2])
    half = 12 * lattice[1]
    tile = lattice[1:]
    hbm = pl.BlockSpec(memory_space=pltpu.HBM)
    vmem = pl.BlockSpec(memory_space=pltpu.VMEM)
    outs = pl.pallas_call(
        functools.partial(kernel, counts),
        out_shape=(pltpu.VMEM(field, F32),) * 2,
        in_specs=[hbm] * 8,
        out_specs=(vmem,) * 2,
        scratch_shapes=[
            pltpu.SMEM(bc_sign.shape, jnp.int32),
            pltpu.SMEM((columns,), jnp.int32),
            pltpu.VMEM(field, F32),
            pltpu.VMEM(field, F32),
            pltpu.VMEM((72 * tall, 128), F32),
            pltpu.VMEM((144 * tall, 128), F32),
            pltpu.VMEM(nulls, jnp.bfloat16),
            pltpu.VMEM(links.shape, F32),
            pltpu.VMEM(field, F32),
            pltpu.VMEM(field, F32),
            pltpu.VMEM((18 * 8, 128), F32),
            pltpu.VMEM((2, 2, half, 128), F32),
            pltpu.VMEM((2, 2, half, 128), F32),
            pltpu.VMEM((2, 2, 12 * T, 128), F32),
            pltpu.VMEM((2, 2, half, 128), F32),
            pltpu.VMEM((2, 2, half, 128), F32),
            pltpu.VMEM((2, 2, 12 * T, 128), F32),
            pltpu.VMEM((half, 128), F32),
            pltpu.VMEM((columns, 48, BLK * BLK, 128), jnp.bfloat16),
            pltpu.VMEM((128 * 8, 128), F32),
            pltpu.VMEM((9, nv) + tile, F32),
            pltpu.VMEM((2, nv) + tile, F32),
            pltpu.VMEM((CITERS,) + tile, F32),
            pltpu.VMEM((CITERS - 1, 6) + tile, F32),
            pltpu.VMEM(tile, F32),
            pltpu.VMEM((128, 128), F32),
            pltpu.VMEM((columns, 3, nv, BLK * BLK, 128), jnp.bfloat16),
            pltpu.VMEM((columns, 24, BLK * BLK, 128), F32),
            pltpu.SemaphoreType.DMA((11,)),
            pltpu.SemaphoreType.DMA((12,)),
            pltpu.SemaphoreType.DMA((12,)),
        ],
        compiler_params=pltpu.CompilerParams(
            collective_id=0, has_side_effects=True, vmem_limit_bytes=66_200_000
        ),
    )(
        bc_sign,
        block_slot.reshape(-1),
        source.reshape(field),
        iterate.reshape(field),
        gauge_links.reshape(72 * tall, 128),
        clover.reshape(144 * tall, 128),
        null_store.reshape(nulls),
        links,
    )
    outs = [pltpu.with_memory_space_constraint(out, pltpu.VMEM) for out in outs]
    outs = pl.pallas_call(
        hand_over,
        out_shape=(jax.ShapeDtypeStruct(field, F32),) * 2,
        in_specs=[vmem] * 2,
        out_specs=(hbm,) * 2,
        scratch_shapes=[pltpu.SemaphoreType.DMA((2,))],
        compiler_params=pltpu.CompilerParams(vmem_limit_bytes=66_200_000),
    )(*outs)
    return tuple(out.reshape(source.shape) for out in outs)


def solution(mesh):
    placed = (
        P(None, None, None, "ta", "gz", "xy"),
        P(None, None, None, "ta", "gz", "xy"),
        P(None, None, None, None, "ta", "gz", "xy"),
        P(None, None, None, None, "ta", "gz", "xy"),
        P(),
        P("ta", "gz", "xy", None, None, None, None, None, None),
        P("ta", "gz", "xy"),
        P(None, None, None, None, "ta", "gz", "xy", None),
    )
    return jax.shard_map(
        functools.partial(per_device, dict(mesh.shape)),
        mesh=mesh,
        in_specs=placed,
        out_specs=(P(None, None, None, "ta", "gz", "xy"), P(None, None, None, "ta", "gz", "xy")),
        check_vma=False,
    )
```

```python
import functools

import jax
import jax.numpy as jnp
from jax import lax
from jax.experimental import pallas as pl
from jax.experimental.pallas import tpu as pltpu
from jax.sharding import PartitionSpec as P

BLK = 4
LY = 32
CITERS = 4
MASS_TERM = 3.8
RELAX_WEIGHT = 0.4
MESH = pl.DeviceIdType.MESH
LANES = 32
F32 = jnp.float32

UPPER = [((0, 0), (1, 0)), ((0, 3), (1, 1)), ((1, 3), (0, 3)), ((1, 2), (0, 0))]
LOWER = [((0, 0), (1, 0)), ((0, 1), (1, 3)), ((1, 1), (0, 1)), ((1, 0), (0, 2))]


def add_turned(a, b, power):
    power %= 4
    if power == 0:
        return (a[0] + b[0], a[1] + b[1])
    if power == 1:
        return (a[0] - b[1], a[1] + b[0])
    if power == 2:
        return (a[0] - b[0], a[1] - b[1])
    return (a[0] + b[1], a[1] - b[0])


def project(psi, mu, forward):
    turn = 2 if forward else 0
    return [
        [add_turned(psi[row][c], psi[2 + UPPER[mu][row][0]][c], UPPER[mu][row][1] + turn) for c in range(3)]
        for row in range(2)
    ]


def rebuild(total, half, mu, forward):
    turn = 2 if forward else 0
    for row in range(2):
        index, power = LOWER[mu][row]
        for c in range(3):
            total[row][c] = add_turned(total[row][c], half[row][c], 0)
            total[2 + row][c] = add_turned(total[2 + row][c], half[index][c], power + turn)


def link_times(link, half):
    out = [[None] * 3 for _ in range(2)]
    for a in range(3):
        for b in range(3):
            ur, ui = link(0, a * 3 + b), link(1, a * 3 + b)
            for s in range(2):
                hr, hi = half[s][b]
                term = (ur * hr - ui * hi, ur * hi + ui * hr)
                out[s][a] = term if b == 0 else add_turned(out[s][a], term, 0)
    return out


def link_dagger(link, half):
    out = [[None] * 3 for _ in range(2)]
    for a in range(3):
        for b in range(3):
            ur, ui = link(0, b * 3 + a), link(1, b * 3 + a)
            for s in range(2):
                hr, hi = half[s][b]
                term = (ur * hr + ui * hi, ur * hi - ui * hr)
                out[s][a] = term if b == 0 else add_turned(out[s][a], term, 0)
    return out


def rows(ref, index, height=8):
    start = index * height
    return ref[pl.ds(start if isinstance(index, int) else pl.multiple_of(start, height), height), :]


def put_rows(ref, index, value, height=8):
    start = index * height
    ref[pl.ds(start if isinstance(index, int) else pl.multiple_of(start, height), height), :] = value


def spinor_of(get):
    return [[(get(s * 3 + c), get(12 + s * 3 + c)) for c in range(3)] for s in range(4)]


def half_of(get):
    return [[(get(s * 3 + c), get(6 + s * 3 + c)) for c in range(3)] for s in range(2)]


def put_half(half, put):
    for s in range(2):
        for c in range(3):
            put(s * 3 + c, half[s][c][0])
            put(6 + s * 3 + c, half[s][c][1])


def map_half(half, change):
    return [[(change(z[0]), change(z[1])) for z in row] for row in half]


def zero_spinor(like):
    return [[(jnp.zeros_like(like), jnp.zeros_like(like)) for _ in range(3)] for _ in range(4)]


def roll(value, shift, axis):
    shift %= value.shape[axis]
    return value if shift == 0 else pltpu.roll(value, shift, axis)


def split_columns(a, b, top):
    return (
        jnp.where(top, a, pltpu.roll(b, BLK, 0)),
        jnp.where(top, pltpu.roll(a, BLK, 0), b),
    )


def wide(a, b):
    return a.astype(F32) * b.astype(F32)


def several(count, step, work):
    def body(g, carry):
        for j in range(step):
            work(g * step + j)
        return carry

    lax.fori_loop(0, count // step, body, 0)


def kernel(
    counts, bc_hbm, slot_hbm, src_hbm, it_hbm, ga_hbm, cl_hbm, nu_hbm, co_hbm, out_it, out_res,
    bc_ref, slot_ref, src, itv, ga, cl, nu, co, res, corr, gx, st, sx, sz, rt, rx, rz, hx, fc, red, pk, part, wbuf,
    wr, rhs, wexp, wv, pc, load_sem, send_sem, recv_sem,
):
    T = BLK
    names = ("ta", "gz", "xy")
    nv = nu.shape[2]

    def load(number, source, target):
        copy = pltpu.make_async_copy(source, target, load_sem.at[number])
        copy.start()
        return copy

    def link_part(ref, mu):
        size = ref.shape[0] // 4
        return ref.at[pl.ds(mu * size, size), :]

    load_it = load(0, it_hbm, itv)
    load_x = load(1, link_part(ga_hbm, 2), link_part(ga, 2))
    place = {n: lax.axis_index(n) for n in names}
    ahead = {n: {n: lax.rem(place[n] + 1, counts[n])} for n in names}
    behind = {n: {n: lax.rem(place[n] + counts[n] - 1, counts[n])} for n in names}
    barrier = pltpu.get_barrier_semaphore()
    for n in ("xy", "ta", "gz"):
        for target in (ahead[n], behind[n]):
            pl.semaphore_signal(barrier, inc=1, device_id=target, device_id_type=MESH)
    load_t = load(2, link_part(ga_hbm, 0), link_part(ga, 0))
    load_z = load(3, link_part(ga_hbm, 1), link_part(ga, 1))
    load_bc = load(4, bc_hbm, bc_ref)
    load_slot = load(5, slot_hbm, slot_ref)

    def message(phase, number, source, target, device):
        slot = (phase % 2) * 6 + number
        return pltpu.make_async_remote_copy(
            src_ref=source, dst_ref=target, send_sem=send_sem.at[number], recv_sem=recv_sem.at[slot],
            device_id=device, device_id_type=MESH,
        )

    def send(*parts):
        copy = message(*parts)
        copy.start()
        return copy

    row = lax.broadcasted_iota(jnp.int32, (8, 128), 0)
    lane = lax.broadcasted_iota(jnp.int32, (8, 128), 1)
    column_y = lane & (LY - 1)
    group = lane // LY
    top = row < BLK

    def gauge(mu, t):
        return lambda ri, m: rows(ga, ((mu * 2 + ri) * 9 + m) * T + t)

    def gauge_edge_z(ri, m):
        return ga[pl.ds((((2 + ri) * 9 + m) * T) * 8 + 7, T, stride=8), :]

    def gauge_edge_x(ri, m):
        return rows(gx, ri * 9 + m)

    def site(field, t):
        return spinor_of(lambda k: rows(field, k * T + t))

    def gathered(values, offset):
        moved = [roll(v, LY * t + offset, 1) for t, v in enumerate(values)]
        value = moved[T - 1]
        for t in range(T - 1):
            value = jnp.where(group == t, moved[t], value)
        return value

    def pack_links():
        for ri in range(2):
            for m in range(9):
                base = (((4 + ri) * 9 + m) * T)
                put_rows(gx, ri * 9 + m, gathered([rows(ga, base + t) for t in range(T)], LY))

    def halo(d, number, name, outgoing, incoming, choice):
        copies = []
        for way in (choice, 1 - choice):
            target = {name: lax.rem(place[name] + counts[name] - 1 + 2 * way, counts[name])}
            copies.append(message(d * 4, number + way, outgoing.at[d, way], incoming.at[d, way], target))
        return copies

    def halos(d):
        return (
            halo(d, 0, "xy", sx, rx, (place["xy"] + 1) // counts["xy"]),
            halo(d, 2, "ta", st, rt, lax.rem(place["ta"], 2)),
            halo(d, 4, "gz", sz, rz, 0),
        )

    def start_all(copies):
        for copy in copies:
            copy.start()

    def fill_x(d, field):
        sites = [site(field, t) for t in range(T)]

        def joined(forward, offset):
            halves = [project(psi, 2, forward) for psi in sites]
            return [
                [tuple(gathered([h[s][c][ri] for h in halves], offset) for ri in range(2)) for c in range(3)]
                for s in range(2)
            ]

        put_half(joined(True, 0), lambda c, v: put_rows(sx.at[d, 0], c, v))
        put_half(link_dagger(gauge_edge_x, joined(False, LY)), lambda c, v: put_rows(sx.at[d, 1], c, v))

    def fill_t(d, field):
        put_half(project(site(field, 0), 0, True), lambda c, v: put_rows(st.at[d, 0], c, v))
        half = link_dagger(gauge(0, T - 1), project(site(field, T - 1), 0, False))
        put_half(half, lambda c, v: put_rows(st.at[d, 1], c, v))

    def fill_z(d, field):
        low = spinor_of(lambda k: field[pl.ds(k * T * 8, T, stride=8), :])
        put_half(project(low, 1, True), lambda c, v: put_rows(sz.at[d, 0], c, v, T))
        high = spinor_of(lambda k: field[pl.ds(k * T * 8 + 7, T, stride=8), :])
        half = link_dagger(gauge_edge_z, project(high, 1, False))
        put_half(half, lambda c, v: put_rows(sz.at[d, 1], c, v, T))

    def local_part(field, base, out, sign_y, before, moved=None):
        def keep(total, t, old):
            for s in range(4):
                for c in range(3):
                    for ri in range(2):
                        at = (ri * 12 + s * 3 + c) * T + t
                        value = 0.5 * total[s][c][ri]
                        put_rows(out, at, rows(out, at) + value if old else value)

        def inside_tile(t, carry):
            psi = site(field, t)
            total = zero_spinor(psi[0][0][0])
            inner = map_half(project(psi, 2, True), lambda v: jnp.where(lane >= 128 - LY, 0.0, roll(v, -LY, 1)))
            rebuild(total, link_times(gauge(2, t), inner), 2, True)
            inner = link_dagger(gauge(2, t), project(psi, 2, False))
            rebuild(total, map_half(inner, lambda v: jnp.where(lane < LY, 0.0, roll(v, LY, 1))), 2, False)
            inner = map_half(project(psi, 1, True), lambda v: jnp.where(row == 7, 0.0, roll(v, -1, 0)))
            rebuild(total, link_times(gauge(1, t), inner), 1, True)
            inner = link_dagger(gauge(1, t), project(psi, 1, False))
            rebuild(total, map_half(inner, lambda v: jnp.where(row == 0, 0.0, roll(v, 1, 0))), 1, False)
            keep(total, t, False)
            return carry

        lax.fori_loop(0, T, inside_tile, 0)
        before[0]()

        def along_t_y(t, carry):
            total = zero_spinor(lane.astype(F32))
            next_t, last_t = lax.rem(t + 1, T), lax.rem(t + T - 1, T)
            inside = jnp.where(t == T - 1, 0.0, 1.0)
            inner = link_times(gauge(0, t), project(site(field, next_t), 0, True))
            rebuild(total, map_half(inner, lambda v: v * inside), 0, True)
            within = jnp.where(t == 0, 0.0, 1.0)
            inner = link_dagger(gauge(0, last_t), project(site(field, last_t), 0, False))
            rebuild(total, map_half(inner, lambda v: v * within), 0, False)
            psi = site(field, t)

            def up(v):
                return jnp.where(column_y == LY - 1, roll(v, LY - 1, 1) * sign_y, roll(v, -1, 1))

            def down(v):
                return jnp.where(column_y == 0, roll(v, 1 - LY, 1) * sign_y, roll(v, 1, 1))

            rebuild(total, link_times(gauge(3, t), map_half(project(psi, 3, True), up)), 3, True)
            rebuild(total, map_half(link_dagger(gauge(3, t), project(psi, 3, False)), down), 3, False)
            keep(total, t, True)
            return carry

        lax.fori_loop(0, T, along_t_y, 0)
        before[1]()

        def on_site(t, carry):
            psi = site(field, t)
            for ch in range(2):
                for i in range(6):
                    s, c = 2 * ch + i // 3, i % 3
                    re, im = psi[s][c][0] * MASS_TERM, psi[s][c][1] * MASS_TERM
                    for j in range(6):
                        vr, vi = psi[2 * ch + j // 3][j % 3]
                        index = (ch * 2 * 36 + i * 6 + j) * T + t
                        mr, mi = rows(cl, index), rows(cl, index + 36 * T)
                        re = re + (mr * vr - mi * vi)
                        im = im + (mr * vi + mi * vr)
                    k = s * 3 + c
                    here, there = k * T + t, (12 + k) * T + t
                    put_rows(out, here, rows(out, here) + rows(base, here) - re)
                    put_rows(out, there, rows(out, there) + rows(base, there) - im)
                    if moved is not None:
                        for at, value in ((here, psi[s][c][0]), (there, psi[s][c][1])):
                            put_rows(moved, at, rows(itv, at) + value)
            return carry

        lax.fori_loop(0, T, on_site, 0)

    def add_to(out, total, where):
        for s in range(4):
            for c in range(3):
                for ri in range(2):
                    spot = where(ri * 12 + s * 3 + c)
                    out[spot] = out[spot] + 0.5 * total[s][c][ri]

    def wait_all(copies):
        for copy in copies:
            copy.wait()

    def far_part(d, out, copies, last, first):
        wait_all(copies[2])
        edge = half_of(lambda c: rows(rz.at[d, 0], c, T) * last[1])
        total = zero_spinor(edge[0][0][0])
        rebuild(total, link_times(gauge_edge_z, edge), 1, True)
        add_to(out, total, lambda k: (pl.ds(k * T * 8 + 7, T, stride=8), slice(None)))
        total = zero_spinor(edge[0][0][0])
        rebuild(total, half_of(lambda c: rows(rz.at[d, 1], c, T) * first[1]), 1, False)
        add_to(out, total, lambda k: (pl.ds(k * T * 8, T, stride=8), slice(None)))
        wait_all(copies[1])
        total = zero_spinor(lane.astype(F32))
        edge = half_of(lambda c: rows(rt.at[d, 0], c) * last[0])
        rebuild(total, link_times(gauge(0, T - 1), edge), 0, True)
        add_to(out, total, lambda k: (pl.ds((k * T + T - 1) * 8, 8), slice(None)))
        total = zero_spinor(lane.astype(F32))
        rebuild(total, half_of(lambda c: rows(rt.at[d, 1], c) * first[0]), 0, False)
        add_to(out, total, lambda k: (pl.ds(k * T * 8, 8), slice(None)))
        wait_all(copies[0])
        edge = half_of(lambda c: rows(rx.at[d, 0], c) * last[2])
        put_half(link_times(gauge_edge_x, edge), lambda c, v: put_rows(hx, c, v))
        way = jnp.where(group == T - 1, -1.0, 1.0)
        for t in range(T):
            def both(c):
                fore = roll(rows(hx, c), -LY * (t + 1), 1)
                back = roll(rows(rx.at[d, 1], c) * first[2], -LY * t, 1)
                return jnp.where(group == T - 1, fore, jnp.where(group == 0, back, 0.0))

            half = half_of(both)
            total = zero_spinor(lane.astype(F32))
            for s in range(2):
                index, power = LOWER[2][s]
                for c in range(3):
                    total[s][c] = half[s][c]
                    z = half[index][c]
                    total[2 + s][c] = add_turned(total[2 + s][c], (z[0] * way, z[1] * way), power)
            add_to(out, total, lambda k: (pl.ds((k * T + t) * 8, 8), slice(None)))

    load_it.wait()
    load_cl = load(0, cl_hbm, cl)
    load_x.wait()
    load_y = load(1, link_part(ga_hbm, 3), link_part(ga, 3))
    pack_links()
    fill_x(0, itv)
    load_t.wait()
    load_src = load(2, src_hbm, src)
    fill_t(0, itv)
    load_z.wait()
    load_nu = load(3, nu_hbm, nu)
    fill_z(0, itv)
    load_bc.wait()
    load_co = load(4, co_hbm, co)
    load_slot.wait()
    red[...] = jnp.zeros(red.shape, F32)
    pl.semaphore_wait(barrier, 6)
    copies = halos(0)
    for group_of in copies:
        start_all(group_of)
    sign = [bc_ref[mu].astype(F32) for mu in range(4)]
    last = [jnp.where(place[n] == counts[n] - 1, sign[i], 1.0) for i, n in enumerate(names)]
    first = [jnp.where(place[n] == 0, sign[i], 1.0) for i, n in enumerate(names)]
    swap = jnp.full((8, 128), slot_ref[0], jnp.int32) != 0

    def ready_site():
        load_src.wait()
        load_cl.wait()

    local_part(itv, src, res, sign[3], (load_y.wait, ready_site))

    def pack_coarse(k, carry):
        for i in range(nv):
            parts = [co[k, ri, i, col] for col in range(2) for ri in range(2)]
            parts = [jnp.concatenate([v, jnp.zeros((8, 128 - nv), F32)], axis=1) for v in parts]
            value = parts[0]
            for g in range(1, 4):
                value = value + roll(parts[g], LANES * g, 1)
            pk[k, i] = value
        return carry

    far_part(0, res, copies, last, first)

    def to_columns(k):
        low, high = [], []
        for pair, group_of in enumerate((low, high)):
            a, b = rows(res, k * T + 2 * pair), rows(res, k * T + 2 * pair + 1)
            col_0, col_1 = split_columns(a, b, top)
            group_of.append(jnp.where(swap, col_1, col_0))
            group_of.append(jnp.where(swap, col_0, col_1))
        for slot in range(2):
            value = jnp.concatenate([low[slot], high[slot]], axis=0).astype(jnp.bfloat16)
            fc[slot, k] = value
            fc[slot, 24 + k] = -value

    several(24, 4, to_columns)
    load_nu.wait()
    for slot in range(2):
        def restrict(g):
            sums = [None] * 4
            for s in range(12):
                fr, fi, minus = fc[slot, s], fc[slot, 12 + s], fc[slot, 24 + s]
                for j in range(2):
                    nr, ni = nu[slot, 0, g * 2 + j, s], nu[slot, 1, g * 2 + j, s]
                    for q, pair in enumerate(((fr, fi), (fi, minus))):
                        at = 2 * j + q
                        term = wide(nr, pair[0])
                        sums[at] = term if sums[at] is None else sums[at] + term
                        sums[at] = sums[at] + wide(ni, pair[1])
            for j in range(2):
                for ri in range(2):
                    value = sums[2 * j + ri]
                    put_rows(red, (2 * slot + ri) * LANES + g * 2 + j, value[:8] + value[8:])

        several(nv // 2, 4, restrict)
    gathered_rows = red[pl.ds(0, 128, stride=8), :]
    for r in range(1, 8):
        gathered_rows = gathered_rows + red[pl.ds(r, 128, stride=8), :]
    turned = jnp.transpose(gathered_rows)
    value = None
    for m in range(4):
        part_sum = turned[8 * m:8 * m + 8]
        for x in range(1, BLK):
            part_sum = part_sum + turned[LY * x + 8 * m:LY * x + 8 * m + 8]
        part_sum = part_sum + roll(part_sum, 1, 0)
        part_sum = part_sum + roll(part_sum, 2, 0)
        lower, upper = roll(part_sum, 2 * m - 3, 0), roll(part_sum, 2 * m + 1 - 7, 0)
        here = jnp.where(row == 2 * m, lower, upper)
        value = here if m == 0 else jnp.where(row // 2 == m, here, value)
    value = jnp.where(swap, roll(value, 2 * LANES, 1), value)
    rhs[...] = value
    wbuf[0] = RELAX_WEIGHT * value

    even = (group & 1) == 0
    turn = jnp.where(even, 1.0, -1.0)

    def pairs_of(w):
        return w * turn, jnp.where(even, roll(w, -LANES, 1), roll(w, LANES, 1))

    def products(vectors, i, sums):
        for k, (wa, wb) in vectors:
            y = pk[k, i]
            sums = (y * wa, y * wb) if sums is None else (sums[0] + y * wa, sums[1] + y * wb)
        return sums

    block = 8
    for it in range(CITERS - 1):
        phase = it + 1
        own = wbuf[it]
        targets = [behind["xy"], ahead["xy"], behind["ta"], ahead["ta"], behind["gz"], ahead["gz"]]
        copies = [send(phase, d, wbuf.at[it], wr.at[it, d], targets[d]) for d in range(6)]
        if it == 0:
            load_co.wait()
            lax.fori_loop(0, 9, pack_coarse, 0)
        vectors = [(0, pairs_of(own)), (7, pairs_of(roll(own, -1, 0))), (8, pairs_of(roll(own, 1, 0)))]

        def near(g, carry):
            for j in range(block):
                i = g * block + j
                part[0, i], part[1, i] = products(vectors, i, None)
            return carry

        lax.fori_loop(0, nv // block, near, 0)
        copies[4].wait()
        copies[5].wait()
        half = 2 * LANES
        next_z = jnp.where(lane < half, roll(own, half, 1), roll(wr[it, 4], half, 1))
        last_z = jnp.where(lane < half, roll(wr[it, 5], half, 1), roll(own, half, 1))
        z_vectors = [(3, pairs_of(next_z)), (4, pairs_of(last_z))]

        def middle(g, carry):
            for j in range(block):
                i = g * block + j
                part[0, i], part[1, i] = products(z_vectors, i, (part[0, i], part[1, i]))
            return carry

        lax.fori_loop(0, nv // block, middle, 0)
        for d in range(4):
            copies[d].wait()
        far_vectors = [(k, pairs_of(wr[it, d])) for k, d in ((1, 2), (2, 3), (5, 0), (6, 1))]
        applied = jnp.zeros((8, 128), F32)
        for i in range(nv):
            sums = products(far_vectors, i, (part[0, i], part[1, i]))
            for ri in range(2):
                for col in range(2):
                    mine = (lane < half) if col == 0 else (lane >= half)
                    whole = jnp.sum(jnp.where(mine, sums[ri], 0.0), axis=1, keepdims=True)
                    applied = jnp.where(lane == LANES * (2 * col + ri) + i, whole, applied)
        wbuf[it + 1] = own + RELAX_WEIGHT * (rhs[...] - (2.0 * own + applied))

    w = wbuf[CITERS - 1]
    w = jnp.where(swap, roll(w, 2 * LANES, 1), w)
    tall = []
    for m in range(4):
        low, high = jnp.broadcast_to(w[2 * m:2 * m + 1], (8, 128)), jnp.broadcast_to(w[2 * m + 1:2 * m + 2], (8, 128))
        tall.append(jnp.where(top, low, high))
    wexp[...] = jnp.transpose(jnp.concatenate(tall * BLK, axis=0))

    def spread(c):
        for slot in range(2):
            values = [wexp[pl.ds((2 * slot + ri) * LANES + c, 1), :] for ri in range(2)]
            for at, v in enumerate((values[0], values[1], -values[1])):
                wv[slot, at, c] = jnp.broadcast_to(v, (2 * 8, 128)).astype(jnp.bfloat16)

    several(nv, 4, spread)
    for slot in range(2):
        def prolong(q, carry):
            sums = [None] * 4
            for c in range(nv):
                vr, vi, minus = wv[slot, 0, c], wv[slot, 1, c], wv[slot, 2, c]
                for j in range(2):
                    nr, ni = nu[slot, 0, c, q * 2 + j], nu[slot, 1, c, q * 2 + j]
                    for ri, pair in enumerate(((vr, minus), (vi, vr))):
                        at = 2 * j + ri
                        term = wide(nr, pair[0])
                        sums[at] = term if sums[at] is None else sums[at] + term
                        sums[at] = sums[at] + wide(ni, pair[1])
            for j in range(2):
                for ri in range(2):
                    pc[slot, ri * 12 + q * 2 + j] = sums[2 * j + ri]
            return carry

        lax.fori_loop(0, 6, prolong, 0)

    def from_columns(k):
        for pair in range(2):
            part_0, part_1 = pc[0, k, pl.ds(8 * pair, 8), :], pc[1, k, pl.ds(8 * pair, 8), :]
            part_0, part_1 = jnp.where(swap, part_1, part_0), jnp.where(swap, part_0, part_1)
            for h, value in enumerate(split_columns(part_0, part_1, top)):
                at = k * T + 2 * pair + h
                put_rows(corr, at, value)

    several(24, 4, from_columns)
    nothing = lambda: None
    copies = halos(1)
    fill_x(1, corr)
    start_all(copies[0])
    fill_t(1, corr)
    start_all(copies[1])
    fill_z(1, corr)
    start_all(copies[2])
    local_part(corr, res, out_res, sign[3], (nothing,) * 2, out_it)
    far_part(1, out_res, copies, last, first)


def hand_over(it_in, res_in, it_out, res_out, sem):
    copies = [
        pltpu.make_async_copy(a, b, sem.at[i]) for i, (a, b) in enumerate(((it_in, it_out), (res_in, res_out)))
    ]
    for copy in copies:
        copy.start()
    for copy in copies:
        copy.wait()


def per_device(counts, source, iterate, gauge_links, clover, bc_sign, null_store, block_slot, coarse_links):
    lattice = source.shape[3:]
    T = lattice[0]
    columns = block_slot.size
    nv = null_store.shape[4]
    assert lattice == (BLK, 2 * BLK, BLK * LY) and columns == 2 and nv % 8 == 0 and nv <= LANES
    nulls = (columns,) + null_store.shape[3:6] + (BLK * BLK, BLK * LY)
    links = jnp.transpose(coarse_links, (0, 1, 2, 4, 5, 6, 7, 3))
    links = links.reshape(links.shape[:3] + (columns,) + links.shape[6:])
    tall = T * lattice[1]
    field = (24 * tall, lattice[2])
    half = 12 * lattice[1]
    tile = lattice[1:]
    hbm = pl.BlockSpec(memory_space=pltpu.HBM)
    vmem = pl.BlockSpec(memory_space=pltpu.VMEM)
    outs = pl.pallas_call(
        functools.partial(kernel, counts),
        out_shape=(pltpu.VMEM(field, F32),) * 2,
        in_specs=[hbm] * 8,
        out_specs=(vmem,) * 2,
        scratch_shapes=[
            pltpu.SMEM(bc_sign.shape, jnp.int32),
            pltpu.SMEM((columns,), jnp.int32),
            pltpu.VMEM(field, F32),
            pltpu.VMEM(field, F32),
            pltpu.VMEM((72 * tall, 128), F32),
            pltpu.VMEM((144 * tall, 128), F32),
            pltpu.VMEM(nulls, jnp.bfloat16),
            pltpu.VMEM(links.shape, F32),
            pltpu.VMEM(field, F32),
            pltpu.VMEM(field, F32),
            pltpu.VMEM((18 * 8, 128), F32),
            pltpu.VMEM((2, 2, half, 128), F32),
            pltpu.VMEM((2, 2, half, 128), F32),
            pltpu.VMEM((2, 2, 12 * T, 128), F32),
            pltpu.VMEM((2, 2, half, 128), F32),
            pltpu.VMEM((2, 2, half, 128), F32),
            pltpu.VMEM((2, 2, 12 * T, 128), F32),
            pltpu.VMEM((half, 128), F32),
            pltpu.VMEM((columns, 48, BLK * BLK, 128), jnp.bfloat16),
            pltpu.VMEM((128 * 8, 128), F32),
            pltpu.VMEM((9, nv) + tile, F32),
            pltpu.VMEM((2, nv) + tile, F32),
            pltpu.VMEM((CITERS,) + tile, F32),
            pltpu.VMEM((CITERS - 1, 6) + tile, F32),
            pltpu.VMEM(tile, F32),
            pltpu.VMEM((128, 128), F32),
            pltpu.VMEM((columns, 3, nv, BLK * BLK, 128), jnp.bfloat16),
            pltpu.VMEM((columns, 24, BLK * BLK, 128), F32),
            pltpu.SemaphoreType.DMA((6,)),
            pltpu.SemaphoreType.DMA((6,)),
            pltpu.SemaphoreType.DMA((12,)),
        ],
        compiler_params=pltpu.CompilerParams(
            collective_id=0, has_side_effects=True, vmem_limit_bytes=66_200_000
        ),
    )(
        bc_sign,
        block_slot.reshape(-1),
        source.reshape(field),
        iterate.reshape(field),
        gauge_links.reshape(72 * tall, 128),
        clover.reshape(144 * tall, 128),
        null_store.reshape(nulls),
        links,
    )
    outs = [pltpu.with_memory_space_constraint(out, pltpu.VMEM) for out in outs]
    outs = pl.pallas_call(
        hand_over,
        out_shape=(jax.ShapeDtypeStruct(field, F32),) * 2,
        in_specs=[vmem] * 2,
        out_specs=(hbm,) * 2,
        scratch_shapes=[pltpu.SemaphoreType.DMA((2,))],
        compiler_params=pltpu.CompilerParams(vmem_limit_bytes=66_200_000),
    )(*outs)
    return tuple(out.reshape(source.shape) for out in outs)


def solution(mesh):
    placed = (
        P(None, None, None, "ta", "gz", "xy"),
        P(None, None, None, "ta", "gz", "xy"),
        P(None, None, None, None, "ta", "gz", "xy"),
        P(None, None, None, None, "ta", "gz", "xy"),
        P(),
        P("ta", "gz", "xy", None, None, None, None, None, None),
        P("ta", "gz", "xy"),
        P(None, None, None, None, "ta", "gz", "xy", None),
    )
    return jax.shard_map(
        functools.partial(per_device, dict(mesh.shape)),
        mesh=mesh,
        in_specs=placed,
        out_specs=(P(None, None, None, "ta", "gz", "xy"), P(None, None, None, "ta", "gz", "xy")),
        check_vma=False,
    )
```

```python
import functools

import jax
import jax.numpy as jnp
from jax import lax
from jax.experimental import pallas as pl
from jax.experimental.pallas import tpu as pltpu
from jax.sharding import PartitionSpec as P

BLK = 4
LY = 32
MASS_TERM = 3.8
RELAX_WEIGHT = 0.4
MESH = pl.DeviceIdType.MESH
LANES = 32
F32 = jnp.float32

UPPER = [((0, 0), (1, 0)), ((0, 3), (1, 1)), ((1, 3), (0, 3)), ((1, 2), (0, 0))]
LOWER = [((0, 0), (1, 0)), ((0, 1), (1, 3)), ((1, 1), (0, 1)), ((1, 0), (0, 2))]


def add_turned(a, b, power):
    power %= 4
    if power == 0:
        return (a[0] + b[0], a[1] + b[1])
    if power == 1:
        return (a[0] - b[1], a[1] + b[0])
    if power == 2:
        return (a[0] - b[0], a[1] - b[1])
    return (a[0] + b[1], a[1] - b[0])


def project(psi, mu, forward):
    turn = 2 if forward else 0
    return [
        [add_turned(psi[row][c], psi[2 + UPPER[mu][row][0]][c], UPPER[mu][row][1] + turn) for c in range(3)]
        for row in range(2)
    ]


def rebuild(total, half, mu, forward):
    turn = 2 if forward else 0
    for row in range(2):
        index, power = LOWER[mu][row]
        for c in range(3):
            total[row][c] = add_turned(total[row][c], half[row][c], 0)
            total[2 + row][c] = add_turned(total[2 + row][c], half[index][c], power + turn)


def link_times(link, half):
    out = [[None] * 3 for _ in range(2)]
    for a in range(3):
        for b in range(3):
            ur, ui = link(0, a * 3 + b), link(1, a * 3 + b)
            for s in range(2):
                hr, hi = half[s][b]
                term = (ur * hr - ui * hi, ur * hi + ui * hr)
                out[s][a] = term if b == 0 else add_turned(out[s][a], term, 0)
    return out


def link_dagger(link, half):
    out = [[None] * 3 for _ in range(2)]
    for a in range(3):
        for b in range(3):
            ur, ui = link(0, b * 3 + a), link(1, b * 3 + a)
            for s in range(2):
                hr, hi = half[s][b]
                term = (ur * hr + ui * hi, ur * hi - ui * hr)
                out[s][a] = term if b == 0 else add_turned(out[s][a], term, 0)
    return out


def rows(ref, index, height=8):
    start = index * height
    return ref[pl.ds(start if isinstance(index, int) else pl.multiple_of(start, height), height), :]


def put_rows(ref, index, value, height=8):
    start = index * height
    ref[pl.ds(start if isinstance(index, int) else pl.multiple_of(start, height), height), :] = value


def spinor_of(get):
    return [[(get(s * 3 + c), get(12 + s * 3 + c)) for c in range(3)] for s in range(4)]


def half_of(get):
    return [[(get(s * 3 + c), get(6 + s * 3 + c)) for c in range(3)] for s in range(2)]


def put_half(half, put):
    for s in range(2):
        for c in range(3):
            put(s * 3 + c, half[s][c][0])
            put(6 + s * 3 + c, half[s][c][1])


def map_half(half, change):
    return [[(change(z[0]), change(z[1])) for z in row] for row in half]


def zero_spinor(like):
    return [[(jnp.zeros_like(like), jnp.zeros_like(like)) for _ in range(3)] for _ in range(4)]


def roll(value, shift, axis):
    shift %= value.shape[axis]
    return value if shift == 0 else pltpu.roll(value, shift, axis)


def split_columns(a, b, top):
    return (
        jnp.where(top, a, pltpu.roll(b, BLK, 0)),
        jnp.where(top, pltpu.roll(a, BLK, 0), b),
    )


def wide(a, b):
    return a.astype(F32) * b.astype(F32)


def several(count, step, work):
    def body(g, carry):
        for j in range(step):
            work(g * step + j)
        return carry

    lax.fori_loop(0, count // step, body, 0)


def kernel(
    counts, bc_hbm, slot_hbm, src_hbm, it_hbm, ga_hbm, cl_hbm, nu_hbm, co_hbm, out_it, out_res,
    bc_ref, slot_ref, src, itv, ga, cl, nu, co, res, corr, gx, st, sx, sz, rt, rx, rz, hx, fc, red, pk, pks, part, wone,
    rh, wr0, wr1, wr2, wmid, fin, zr, zfin, wexp, wv, pc, load_sem, send_sem, recv_sem,
):
    T = BLK
    names = ("ta", "gz", "xy")
    nv = nu.shape[2]

    def load(number, source, target):
        copy = pltpu.make_async_copy(source, target, load_sem.at[number])
        copy.start()
        return copy

    def link_part(ref, mu):
        size = ref.shape[0] // 4
        return ref.at[pl.ds(mu * size, size), :]

    load_it = load(0, it_hbm, itv)
    load_x = load(1, link_part(ga_hbm, 2), link_part(ga, 2))
    place = {n: lax.axis_index(n) for n in names}
    depth = counts["gz"]
    core = lax.rem(place["gz"], 2)
    several_pairs = depth > 2

    def along_z(step):
        return {"gz": lax.rem(place["gz"] + depth + step, depth)}

    def pair_of(other):
        return {"gz": place["gz"] - core + other}

    def away(name, step, other):
        return {name: lax.rem(place[name] + counts[name] + step, counts[name]), **pair_of(other)}

    ways = (("xy", -1), ("xy", 1), ("ta", -1), ("ta", 1))
    greeted = [away(name, step, other) for name, step in ways for other in range(2)]
    greeted += [along_z(step) for step in ((-1, 1, -2, 2) if several_pairs else (1,))]
    barrier = pltpu.get_barrier_semaphore()
    for target in greeted:
        pl.semaphore_signal(barrier, inc=1, device_id=target, device_id_type=MESH)
    load_t = load(2, link_part(ga_hbm, 0), link_part(ga, 0))
    load_z = load(3, link_part(ga_hbm, 1), link_part(ga, 1))
    load_bc = load(4, bc_hbm, bc_ref)
    load_slot = load(5, slot_hbm, slot_ref)

    def message(sent, arrived, source, target, device):
        return pltpu.make_async_remote_copy(
            src_ref=source, dst_ref=target, send_sem=send_sem.at[sent], recv_sem=recv_sem.at[arrived],
            device_id=device, device_id_type=MESH,
        )

    def await_bytes(sem, shaped):
        pltpu.make_async_copy(shaped, shaped, sem).wait()

    row = lax.broadcasted_iota(jnp.int32, (8, 128), 0)
    lane = lax.broadcasted_iota(jnp.int32, (8, 128), 1)
    column_y = lane & (LY - 1)
    group = lane // LY
    top = row < BLK

    def gauge(mu, t):
        return lambda ri, m: rows(ga, ((mu * 2 + ri) * 9 + m) * T + t)

    def gauge_edge_z(ri, m):
        return ga[pl.ds((((2 + ri) * 9 + m) * T) * 8 + 7, T, stride=8), :]

    def gauge_edge_x(ri, m):
        return rows(gx, ri * 9 + m)

    def site(field, t):
        return spinor_of(lambda k: rows(field, k * T + t))

    def gathered(values, offset):
        moved = [roll(v, LY * t + offset, 1) for t, v in enumerate(values)]
        value = moved[T - 1]
        for t in range(T - 1):
            value = jnp.where(group == t, moved[t], value)
        return value

    def pack_links():
        for ri in range(2):
            for m in range(9):
                base = (((4 + ri) * 9 + m) * T)
                put_rows(gx, ri * 9 + m, gathered([rows(ga, base + t) for t in range(T)], LY))

    def halo(d, number, name, outgoing, incoming, choice):
        copies = []
        for way in (choice, 1 - choice):
            target = {name: lax.rem(place[name] + counts[name] - 1 + 2 * way, counts[name])}
            copies.append(message(number + way, number + way, outgoing.at[d, way], incoming.at[d, way], target))
        return copies

    def halos(d):
        return (
            halo(d, 0, "xy", sx, rx, (place["xy"] + 1) // counts["xy"]),
            halo(d, 2, "ta", st, rt, lax.rem(place["ta"], 2)),
            halo(d, 4, "gz", sz, rz, 0),
        )

    def start_all(copies):
        for copy in copies:
            copy.start()

    def fill_x(d, field):
        sites = [site(field, t) for t in range(T)]

        def joined(forward, offset):
            halves = [project(psi, 2, forward) for psi in sites]
            return [
                [tuple(gathered([h[s][c][ri] for h in halves], offset) for ri in range(2)) for c in range(3)]
                for s in range(2)
            ]

        put_half(joined(True, 0), lambda c, v: put_rows(sx.at[d, 0], c, v))
        put_half(link_dagger(gauge_edge_x, joined(False, LY)), lambda c, v: put_rows(sx.at[d, 1], c, v))

    def fill_t(d, field):
        put_half(project(site(field, 0), 0, True), lambda c, v: put_rows(st.at[d, 0], c, v))
        half = link_dagger(gauge(0, T - 1), project(site(field, T - 1), 0, False))
        put_half(half, lambda c, v: put_rows(st.at[d, 1], c, v))

    def fill_z(d, field):
        low = spinor_of(lambda k: field[pl.ds(k * T * 8, T, stride=8), :])
        put_half(project(low, 1, True), lambda c, v: put_rows(sz.at[d, 0], c, v, T))
        high = spinor_of(lambda k: field[pl.ds(k * T * 8 + 7, T, stride=8), :])
        half = link_dagger(gauge_edge_z, project(high, 1, False))
        put_half(half, lambda c, v: put_rows(sz.at[d, 1], c, v, T))

    def local_part(field, base, out, sign_y, before, moved=None):
        def keep(total, t, old):
            for s in range(4):
                for c in range(3):
                    for ri in range(2):
                        at = (ri * 12 + s * 3 + c) * T + t
                        value = 0.5 * total[s][c][ri]
                        put_rows(out, at, rows(out, at) + value if old else value)

        def inside_tile(t, carry):
            psi = site(field, t)
            total = zero_spinor(psi[0][0][0])
            inner = map_half(project(psi, 2, True), lambda v: jnp.where(lane >= 128 - LY, 0.0, roll(v, -LY, 1)))
            rebuild(total, link_times(gauge(2, t), inner), 2, True)
            inner = link_dagger(gauge(2, t), project(psi, 2, False))
            rebuild(total, map_half(inner, lambda v: jnp.where(lane < LY, 0.0, roll(v, LY, 1))), 2, False)
            inner = map_half(project(psi, 1, True), lambda v: jnp.where(row == 7, 0.0, roll(v, -1, 0)))
            rebuild(total, link_times(gauge(1, t), inner), 1, True)
            inner = link_dagger(gauge(1, t), project(psi, 1, False))
            rebuild(total, map_half(inner, lambda v: jnp.where(row == 0, 0.0, roll(v, 1, 0))), 1, False)
            keep(total, t, False)
            return carry

        lax.fori_loop(0, T, inside_tile, 0)
        before[0]()

        def along_t_y(t, carry):
            total = zero_spinor(lane.astype(F32))
            next_t, last_t = lax.rem(t + 1, T), lax.rem(t + T - 1, T)
            inside = jnp.where(t == T - 1, 0.0, 1.0)
            inner = link_times(gauge(0, t), project(site(field, next_t), 0, True))
            rebuild(total, map_half(inner, lambda v: v * inside), 0, True)
            within = jnp.where(t == 0, 0.0, 1.0)
            inner = link_dagger(gauge(0, last_t), project(site(field, last_t), 0, False))
            rebuild(total, map_half(inner, lambda v: v * within), 0, False)
            psi = site(field, t)

            def up(v):
                return jnp.where(column_y == LY - 1, roll(v, LY - 1, 1) * sign_y, roll(v, -1, 1))

            def down(v):
                return jnp.where(column_y == 0, roll(v, 1 - LY, 1) * sign_y, roll(v, 1, 1))

            rebuild(total, link_times(gauge(3, t), map_half(project(psi, 3, True), up)), 3, True)
            rebuild(total, map_half(link_dagger(gauge(3, t), project(psi, 3, False)), down), 3, False)
            keep(total, t, True)
            return carry

        lax.fori_loop(0, T, along_t_y, 0)
        before[1]()

        def on_site(t, carry):
            psi = site(field, t)
            for ch in range(2):
                for i in range(6):
                    s, c = 2 * ch + i // 3, i % 3
                    re, im = psi[s][c][0] * MASS_TERM, psi[s][c][1] * MASS_TERM
                    for j in range(6):
                        vr, vi = psi[2 * ch + j // 3][j % 3]
                        index = (ch * 2 * 36 + i * 6 + j) * T + t
                        mr, mi = rows(cl, index), rows(cl, index + 36 * T)
                        re = re + (mr * vr - mi * vi)
                        im = im + (mr * vi + mi * vr)
                    k = s * 3 + c
                    here, there = k * T + t, (12 + k) * T + t
                    put_rows(out, here, rows(out, here) + rows(base, here) - re)
                    put_rows(out, there, rows(out, there) + rows(base, there) - im)
                    if moved is not None:
                        for at, value in ((here, psi[s][c][0]), (there, psi[s][c][1])):
                            put_rows(moved, at, rows(itv, at) + value)
            return carry

        lax.fori_loop(0, T, on_site, 0)

    def add_to(out, total, where):
        for s in range(4):
            for c in range(3):
                for ri in range(2):
                    spot = where(ri * 12 + s * 3 + c)
                    out[spot] = out[spot] + 0.5 * total[s][c][ri]

    def wait_all(copies):
        for copy in copies:
            copy.wait()

    def far_part(d, out, copies, last, first):
        wait_all(copies[2])
        edge = half_of(lambda c: rows(rz.at[d, 0], c, T) * last[1])
        total = zero_spinor(edge[0][0][0])
        rebuild(total, link_times(gauge_edge_z, edge), 1, True)
        add_to(out, total, lambda k: (pl.ds(k * T * 8 + 7, T, stride=8), slice(None)))
        total = zero_spinor(edge[0][0][0])
        rebuild(total, half_of(lambda c: rows(rz.at[d, 1], c, T) * first[1]), 1, False)
        add_to(out, total, lambda k: (pl.ds(k * T * 8, T, stride=8), slice(None)))
        wait_all(copies[1])
        total = zero_spinor(lane.astype(F32))
        edge = half_of(lambda c: rows(rt.at[d, 0], c) * last[0])
        rebuild(total, link_times(gauge(0, T - 1), edge), 0, True)
        add_to(out, total, lambda k: (pl.ds((k * T + T - 1) * 8, 8), slice(None)))
        total = zero_spinor(lane.astype(F32))
        rebuild(total, half_of(lambda c: rows(rt.at[d, 1], c) * first[0]), 0, False)
        add_to(out, total, lambda k: (pl.ds(k * T * 8, 8), slice(None)))
        wait_all(copies[0])
        edge = half_of(lambda c: rows(rx.at[d, 0], c) * last[2])
        put_half(link_times(gauge_edge_x, edge), lambda c, v: put_rows(hx, c, v))
        way = jnp.where(group == T - 1, -1.0, 1.0)
        for t in range(T):
            def both(c):
                fore = roll(rows(hx, c), -LY * (t + 1), 1)
                back = roll(rows(rx.at[d, 1], c) * first[2], -LY * t, 1)
                return jnp.where(group == T - 1, fore, jnp.where(group == 0, back, 0.0))

            half = half_of(both)
            total = zero_spinor(lane.astype(F32))
            for s in range(2):
                index, power = LOWER[2][s]
                for c in range(3):
                    total[s][c] = half[s][c]
                    z = half[index][c]
                    total[2 + s][c] = add_turned(total[2 + s][c], (z[0] * way, z[1] * way), power)
            add_to(out, total, lambda k: (pl.ds((k * T + t) * 8, 8), slice(None)))

    load_it.wait()
    load_cl = load(0, cl_hbm, cl)
    load_x.wait()
    load_y = load(1, link_part(ga_hbm, 3), link_part(ga, 3))
    pack_links()
    fill_x(0, itv)
    load_t.wait()
    load_src = load(2, src_hbm, src)
    fill_t(0, itv)
    load_z.wait()
    load_co = load(3, co_hbm, co)
    fill_z(0, itv)
    load_bc.wait()
    load_nu = load(4, nu_hbm, nu)
    load_slot.wait()
    red[...] = jnp.zeros(red.shape, F32)
    pl.semaphore_wait(barrier, len(greeted))
    copies = halos(0)
    for group_of in copies:
        start_all(group_of)
    sign = [bc_ref[mu].astype(F32) for mu in range(4)]
    last = [jnp.where(place[n] == counts[n] - 1, sign[i], 1.0) for i, n in enumerate(names)]
    first = [jnp.where(place[n] == 0, sign[i], 1.0) for i, n in enumerate(names)]
    swap = jnp.full((8, 128), slot_ref[0], jnp.int32) != 0

    def ready_site():
        load_src.wait()
        load_cl.wait()

    local_part(itv, src, res, sign[3], (load_y.wait, ready_site))

    def pack_coarse(k, carry):
        for i in range(nv):
            parts = [co[k, ri, i, col] for col in range(2) for ri in range(2)]
            parts = [jnp.concatenate([v, jnp.zeros((8, 128 - nv), F32)], axis=1) for v in parts]
            value = parts[0]
            for g in range(1, 4):
                value = value + roll(parts[g], LANES * g, 1)
            pk[k, i] = value
        return carry

    load_co.wait()
    lax.fori_loop(0, 9, pack_coarse, 0)

    @pl.when(core == 0)
    def _():
        message(6, 8, pk, pks, pair_of(1)).start()

    far_part(0, res, copies, last, first)

    def to_columns(k):
        low, high = [], []
        for pair, group_of in enumerate((low, high)):
            a, b = rows(res, k * T + 2 * pair), rows(res, k * T + 2 * pair + 1)
            col_0, col_1 = split_columns(a, b, top)
            group_of.append(jnp.where(swap, col_1, col_0))
            group_of.append(jnp.where(swap, col_0, col_1))
        for slot in range(2):
            value = jnp.concatenate([low[slot], high[slot]], axis=0).astype(jnp.bfloat16)
            fc[slot, k] = value
            fc[slot, 24 + k] = -value

    several(24, 4, to_columns)
    load_nu.wait()
    for slot in range(2):
        def restrict(g):
            sums = [None] * 4
            for s in range(12):
                fr, fi, minus = fc[slot, s], fc[slot, 12 + s], fc[slot, 24 + s]
                for j in range(2):
                    nr, ni = nu[slot, 0, g * 2 + j, s], nu[slot, 1, g * 2 + j, s]
                    for q, pair in enumerate(((fr, fi), (fi, minus))):
                        at = 2 * j + q
                        term = wide(nr, pair[0])
                        sums[at] = term if sums[at] is None else sums[at] + term
                        sums[at] = sums[at] + wide(ni, pair[1])
            for j in range(2):
                for ri in range(2):
                    value = sums[2 * j + ri]
                    put_rows(red, (2 * slot + ri) * LANES + g * 2 + j, value[:8] + value[8:])

        several(nv // 2, 4, restrict)
    gathered_rows = red[pl.ds(0, 128, stride=8), :]
    for r in range(1, 8):
        gathered_rows = gathered_rows + red[pl.ds(r, 128, stride=8), :]
    turned = jnp.transpose(gathered_rows)
    value = None
    for m in range(4):
        part_sum = turned[8 * m:8 * m + 8]
        for x in range(1, BLK):
            part_sum = part_sum + turned[LY * x + 8 * m:LY * x + 8 * m + 8]
        part_sum = part_sum + roll(part_sum, 1, 0)
        part_sum = part_sum + roll(part_sum, 2, 0)
        lower, upper = roll(part_sum, 2 * m - 3, 0), roll(part_sum, 2 * m + 1 - 7, 0)
        here = jnp.where(row == 2 * m, lower, upper)
        value = here if m == 0 else jnp.where(row // 2 == m, here, value)
    value = jnp.where(swap, roll(value, 2 * LANES, 1), value)
    rh[1] = value
    wone[...] = RELAX_WEIGHT * value
    for d, (name, step) in enumerate(ways):
        message(0, 6, wone, wr0.at[core, d], away(name, step, 1)).start()
    if several_pairs:
        message(7, 10, wone, zr.at[0, 1 - core], along_z(3 * core - 1)).start()

    even = (group & 1) == 0
    turn = jnp.where(even, 1.0, -1.0)
    half = 2 * LANES
    block = 8

    def pairs_of(w):
        return w * turn, jnp.where(even, roll(w, -LANES, 1), roll(w, LANES, 1))

    def products(table, vectors, i, sums):
        for k, (wa, wb) in vectors:
            y = table[k, i]
            sums = (y * wa, y * wb) if sums is None else (sums[0] + y * wa, sums[1] + y * wb)
        return sums

    def near(table, own, above, below, h):
        turned = roll(own, half, 1)
        next_z = jnp.where(lane < half, turned, roll(above, half, 1))
        last_z = jnp.where(lane < half, roll(below, half, 1), turned)
        places = ((0, own), (7, roll(own, -1, 0)), (8, roll(own, 1, 0)), (3, next_z), (4, last_z))
        vectors = [(k, pairs_of(w)) for k, w in places]

        def body(g, carry):
            for j in range(block):
                i = g * block + j
                part[h, 0, i], part[h, 1, i] = products(table, vectors, i, None)
            return carry

        lax.fori_loop(0, nv // block, body, 0)

    def far(table, arrived, own, known, h):
        vectors = [(k, pairs_of(arrived[d])) for k, d in ((1, 2), (2, 3), (5, 0), (6, 1))]
        applied = jnp.zeros((8, 128), F32)
        for i in range(nv):
            sums = products(table, vectors, i, (part[h, 0, i], part[h, 1, i]))
            for ri in range(2):
                for col in range(2):
                    mine = (lane < half) if col == 0 else (lane >= half)
                    whole = jnp.sum(jnp.where(mine, sums[ri], 0.0), axis=1, keepdims=True)
                    applied = jnp.where(lane == LANES * (2 * col + ri) + i, whole, applied)
        return own + RELAX_WEIGHT * (known - (2.0 * own + applied))

    @pl.when(core == 0)
    def _():
        message(0, 7, rh.at[1], rh.at[0], pair_of(1)).start()

    @pl.when(core == 1)
    def _():
        tables = (pks, pk)
        await_bytes(recv_sem.at[7], rh.at[0])
        wmid[0, 0] = RELAX_WEIGHT * rh[0]
        wmid[0, 1] = wone[...]
        await_bytes(recv_sem.at[8], pks)
        for it in range(2):
            if it == 1:
                for d, (name, step) in enumerate(ways):
                    message(0, 9, wmid.at[1], wr1.at[d], away(name, step, 1)).start()
                if several_pairs:
                    message(7, 11, wmid.at[1, 0], zr.at[1, 1], along_z(-2)).start()
                    message(7, 11, wmid.at[1, 1], zr.at[1, 0], along_z(2)).start()
            lower, upper = wmid[it, 0], wmid[it, 1]
            below, above = upper, lower
            if several_pairs:
                await_bytes(recv_sem.at[10 + it], zr.at[it])
                below, above = zr[it, 0], zr[it, 1]
            near(tables[0], lower, upper, below, 0)
            near(tables[1], upper, above, lower, 1)
            if it == 0:
                await_bytes(recv_sem.at[6], wr0)
            else:
                await_bytes(recv_sem.at[9], wr1)
            for h in range(2):
                arrived = [wr0[h, d] if it == 0 else wr1[d, h] for d in range(4)]
                wmid[it + 1, h] = far(tables[h], arrived, wmid[it, h], rh[h], h)
        for d, (name, step) in enumerate(ways):
            message(0, 6, wmid.at[2, 0], wr2.at[d], away(name, step, 0)).start()
        message(0, 7, wmid.at[2], fin, pair_of(0)).start()
        for d, (name, step) in enumerate(ways):
            message(0, 6, wmid.at[2, 1], wr2.at[d], away(name, step, 1)).start()
        if several_pairs:
            message(7, 12, wmid.at[2, 1], zfin, along_z(1)).start()
            message(7, 12, wmid.at[2, 0], zfin, along_z(-2)).start()
        fin[0] = wmid[2, 1]
        fin[1] = wmid[2, 0]

    @pl.when(core == 0)
    def _():
        await_bytes(recv_sem.at[7], fin)

    own, above, below = fin[0], fin[1], fin[1]
    if several_pairs:
        await_bytes(recv_sem.at[12], zfin)
        above, below = jnp.where(core == 0, above, zfin[...]), jnp.where(core == 0, zfin[...], below)
    near(pk, own, above, below, 0)
    await_bytes(recv_sem.at[6], wr2)
    w = far(pk, [wr2[d] for d in range(4)], own, rh[1], 0)

    @pl.when(core == 0)
    def _():
        await_bytes(send_sem.at[0], pk.at[0, pl.ds(0, 5)])
        await_bytes(send_sem.at[6], pk)
        if several_pairs:
            await_bytes(send_sem.at[7], wone)

    @pl.when(core == 1)
    def _():
        await_bytes(send_sem.at[0], pk.at[0, pl.ds(0, 22)])
        if several_pairs:
            await_bytes(send_sem.at[7], pk.at[0, pl.ds(0, 5)])

    w = jnp.where(swap, roll(w, 2 * LANES, 1), w)
    tall = []
    for m in range(4):
        low, high = jnp.broadcast_to(w[2 * m:2 * m + 1], (8, 128)), jnp.broadcast_to(w[2 * m + 1:2 * m + 2], (8, 128))
        tall.append(jnp.where(top, low, high))
    wexp[...] = jnp.transpose(jnp.concatenate(tall * BLK, axis=0))

    def spread(c):
        for slot in range(2):
            values = [wexp[pl.ds((2 * slot + ri) * LANES + c, 1), :] for ri in range(2)]
            for at, v in enumerate((values[0], values[1], -values[1])):
                wv[slot, at, c] = jnp.broadcast_to(v, (2 * 8, 128)).astype(jnp.bfloat16)

    several(nv, 4, spread)
    for slot in range(2):
        def prolong(q, carry):
            sums = [None] * 4
            for c in range(nv):
                vr, vi, minus = wv[slot, 0, c], wv[slot, 1, c], wv[slot, 2, c]
                for j in range(2):
                    nr, ni = nu[slot, 0, c, q * 2 + j], nu[slot, 1, c, q * 2 + j]
                    for ri, pair in enumerate(((vr, minus), (vi, vr))):
                        at = 2 * j + ri
                        term = wide(nr, pair[0])
                        sums[at] = term if sums[at] is None else sums[at] + term
                        sums[at] = sums[at] + wide(ni, pair[1])
            for j in range(2):
                for ri in range(2):
                    pc[slot, ri * 12 + q * 2 + j] = sums[2 * j + ri]
            return carry

        lax.fori_loop(0, 6, prolong, 0)

    def from_columns(k):
        for pair in range(2):
            part_0, part_1 = pc[0, k, pl.ds(8 * pair, 8), :], pc[1, k, pl.ds(8 * pair, 8), :]
            part_0, part_1 = jnp.where(swap, part_1, part_0), jnp.where(swap, part_0, part_1)
            for h, value in enumerate(split_columns(part_0, part_1, top)):
                at = k * T + 2 * pair + h
                put_rows(corr, at, value)

    several(24, 4, from_columns)
    nothing = lambda: None
    copies = halos(1)
    fill_x(1, corr)
    start_all(copies[0])
    fill_t(1, corr)
    start_all(copies[1])
    fill_z(1, corr)
    start_all(copies[2])
    local_part(corr, res, out_res, sign[3], (nothing,) * 2, out_it)
    far_part(1, out_res, copies, last, first)


def hand_over(it_in, res_in, it_out, res_out, sem):
    copies = [
        pltpu.make_async_copy(a, b, sem.at[i]) for i, (a, b) in enumerate(((it_in, it_out), (res_in, res_out)))
    ]
    for copy in copies:
        copy.start()
    for copy in copies:
        copy.wait()


def per_device(counts, source, iterate, gauge_links, clover, bc_sign, null_store, block_slot, coarse_links):
    lattice = source.shape[3:]
    T = lattice[0]
    columns = block_slot.size
    nv = null_store.shape[4]
    assert lattice == (BLK, 2 * BLK, BLK * LY) and columns == 2 and nv % 8 == 0 and nv <= LANES
    nulls = (columns,) + null_store.shape[3:6] + (BLK * BLK, BLK * LY)
    links = jnp.transpose(coarse_links, (0, 1, 2, 4, 5, 6, 7, 3))
    links = links.reshape(links.shape[:3] + (columns,) + links.shape[6:])
    tall = T * lattice[1]
    field = (24 * tall, lattice[2])
    half = 12 * lattice[1]
    tile = lattice[1:]
    hbm = pl.BlockSpec(memory_space=pltpu.HBM)
    vmem = pl.BlockSpec(memory_space=pltpu.VMEM)
    outs = pl.pallas_call(
        functools.partial(kernel, counts),
        out_shape=(pltpu.VMEM(field, F32),) * 2,
        in_specs=[hbm] * 8,
        out_specs=(vmem,) * 2,
        scratch_shapes=[
            pltpu.SMEM(bc_sign.shape, jnp.int32),
            pltpu.SMEM((columns,), jnp.int32),
            pltpu.VMEM(field, F32),
            pltpu.VMEM(field, F32),
            pltpu.VMEM((72 * tall, 128), F32),
            pltpu.VMEM((144 * tall, 128), F32),
            pltpu.VMEM(nulls, jnp.bfloat16),
            pltpu.VMEM(links.shape, F32),
            pltpu.VMEM(field, F32),
            pltpu.VMEM(field, F32),
            pltpu.VMEM((18 * 8, 128), F32),
            pltpu.VMEM((2, 2, half, 128), F32),
            pltpu.VMEM((2, 2, half, 128), F32),
            pltpu.VMEM((2, 2, 12 * T, 128), F32),
            pltpu.VMEM((2, 2, half, 128), F32),
            pltpu.VMEM((2, 2, half, 128), F32),
            pltpu.VMEM((2, 2, 12 * T, 128), F32),
            pltpu.VMEM((half, 128), F32),
            pltpu.VMEM((columns, 48, BLK * BLK, 128), jnp.bfloat16),
            pltpu.VMEM((128 * 8, 128), F32),
            pltpu.VMEM((9, nv) + tile, F32),
            pltpu.VMEM((9, nv) + tile, F32),
            pltpu.VMEM((2, 2, nv) + tile, F32),
            pltpu.VMEM(tile, F32),
            pltpu.VMEM((2,) + tile, F32),
            pltpu.VMEM((2, 4) + tile, F32),
            pltpu.VMEM((4, 2) + tile, F32),
            pltpu.VMEM((4,) + tile, F32),
            pltpu.VMEM((3, 2) + tile, F32),
            pltpu.VMEM((2,) + tile, F32),
            pltpu.VMEM((2, 2) + tile, F32),
            pltpu.VMEM(tile, F32),
            pltpu.VMEM((128, 128), F32),
            pltpu.VMEM((columns, 3, nv, BLK * BLK, 128), jnp.bfloat16),
            pltpu.VMEM((columns, 24, BLK * BLK, 128), F32),
            pltpu.SemaphoreType.DMA((6,)),
            pltpu.SemaphoreType.DMA((8 if counts["gz"] > 2 else 7,)),
            pltpu.SemaphoreType.DMA((13 if counts["gz"] > 2 else 10,)),
        ],
        compiler_params=pltpu.CompilerParams(
            collective_id=0, has_side_effects=True, vmem_limit_bytes=66_200_000
        ),
    )(
        bc_sign,
        block_slot.reshape(-1),
        source.reshape(field),
        iterate.reshape(field),
        gauge_links.reshape(72 * tall, 128),
        clover.reshape(144 * tall, 128),
        null_store.reshape(nulls),
        links,
    )
    outs = [pltpu.with_memory_space_constraint(out, pltpu.VMEM) for out in outs]
    outs = pl.pallas_call(
        hand_over,
        out_shape=(jax.ShapeDtypeStruct(field, F32),) * 2,
        in_specs=[vmem] * 2,
        out_specs=(hbm,) * 2,
        scratch_shapes=[pltpu.SemaphoreType.DMA((2,))],
        compiler_params=pltpu.CompilerParams(vmem_limit_bytes=66_200_000),
    )(*outs)
    return tuple(out.reshape(source.shape) for out in outs)


def solution(mesh):
    placed = (
        P(None, None, None, "ta", "gz", "xy"),
        P(None, None, None, "ta", "gz", "xy"),
        P(None, None, None, None, "ta", "gz", "xy"),
        P(None, None, None, None, "ta", "gz", "xy"),
        P(),
        P("ta", "gz", "xy", None, None, None, None, None, None),
        P("ta", "gz", "xy"),
        P(None, None, None, None, "ta", "gz", "xy", None),
    )
    return jax.shard_map(
        functools.partial(per_device, dict(mesh.shape)),
        mesh=mesh,
        in_specs=placed,
        out_specs=(P(None, None, None, "ta", "gz", "xy"), P(None, None, None, "ta", "gz", "xy")),
        check_vma=False,
    )
```

```python
import functools

import jax
import jax.numpy as jnp
from jax import lax
from jax.experimental import pallas as pl
from jax.experimental.pallas import tpu as pltpu
from jax.sharding import PartitionSpec as P

BLK = 4
LY = 32
MASS_TERM = 3.8
RELAX_WEIGHT = 0.4
MESH = pl.DeviceIdType.MESH
LANES = 32
F32 = jnp.float32

UPPER = [((0, 0), (1, 0)), ((0, 3), (1, 1)), ((1, 3), (0, 3)), ((1, 2), (0, 0))]
LOWER = [((0, 0), (1, 0)), ((0, 1), (1, 3)), ((1, 1), (0, 1)), ((1, 0), (0, 2))]


def add_turned(a, b, power):
    power %= 4
    if power == 0:
        return (a[0] + b[0], a[1] + b[1])
    if power == 1:
        return (a[0] - b[1], a[1] + b[0])
    if power == 2:
        return (a[0] - b[0], a[1] - b[1])
    return (a[0] + b[1], a[1] - b[0])


def project(psi, mu, forward):
    turn = 2 if forward else 0
    return [
        [add_turned(psi[row][c], psi[2 + UPPER[mu][row][0]][c], UPPER[mu][row][1] + turn) for c in range(3)]
        for row in range(2)
    ]


def rebuild(total, half, mu, forward):
    turn = 2 if forward else 0
    for row in range(2):
        index, power = LOWER[mu][row]
        for c in range(3):
            total[row][c] = add_turned(total[row][c], half[row][c], 0)
            total[2 + row][c] = add_turned(total[2 + row][c], half[index][c], power + turn)


def link_times(link, half):
    out = [[None] * 3 for _ in range(2)]
    for a in range(3):
        for b in range(3):
            ur, ui = link(0, a * 3 + b), link(1, a * 3 + b)
            for s in range(2):
                hr, hi = half[s][b]
                term = (ur * hr - ui * hi, ur * hi + ui * hr)
                out[s][a] = term if b == 0 else add_turned(out[s][a], term, 0)
    return out


def link_dagger(link, half):
    out = [[None] * 3 for _ in range(2)]
    for a in range(3):
        for b in range(3):
            ur, ui = link(0, b * 3 + a), link(1, b * 3 + a)
            for s in range(2):
                hr, hi = half[s][b]
                term = (ur * hr + ui * hi, ur * hi - ui * hr)
                out[s][a] = term if b == 0 else add_turned(out[s][a], term, 0)
    return out


def rows(ref, index, height=8):
    start = index * height
    return ref[pl.ds(start if isinstance(index, int) else pl.multiple_of(start, height), height), :]


def put_rows(ref, index, value, height=8):
    start = index * height
    ref[pl.ds(start if isinstance(index, int) else pl.multiple_of(start, height), height), :] = value


def spinor_of(get):
    return [[(get(s * 3 + c), get(12 + s * 3 + c)) for c in range(3)] for s in range(4)]


def half_of(get):
    return [[(get(s * 3 + c), get(6 + s * 3 + c)) for c in range(3)] for s in range(2)]


def put_half(half, put):
    for s in range(2):
        for c in range(3):
            put(s * 3 + c, half[s][c][0])
            put(6 + s * 3 + c, half[s][c][1])


def map_half(half, change):
    return [[(change(z[0]), change(z[1])) for z in row] for row in half]


def zero_spinor(like):
    return [[(jnp.zeros_like(like), jnp.zeros_like(like)) for _ in range(3)] for _ in range(4)]


def roll(value, shift, axis):
    shift %= value.shape[axis]
    return value if shift == 0 else pltpu.roll(value, shift, axis)


def split_columns(a, b, top):
    return (
        jnp.where(top, a, pltpu.roll(b, BLK, 0)),
        jnp.where(top, pltpu.roll(a, BLK, 0), b),
    )


def wide(a, b):
    return a.astype(F32) * b.astype(F32)


def several(count, step, work):
    def body(g, carry):
        for j in range(step):
            work(g * step + j)
        return carry

    lax.fori_loop(0, count // step, body, 0)


def kernel(
    counts, bc_hbm, slot_hbm, src_hbm, it_hbm, ga_hbm, cl_hbm, nu_hbm, co_hbm, out_it, out_res,
    bc_ref, slot_ref, src, itv, ga, cl, nu, co, res, corr, gx, st, sx, sz, rt, rx, rz, hx, fc, red, pk, pks, part, wone,
    rh, wr0, wr1, wr2, wmid, fin, zr, zfin, wexp, wv, pc, load_sem, send_sem, recv_sem,
):
    T = BLK
    names = ("ta", "gz", "xy")
    nv = nu.shape[2]

    def load(number, source, target):
        copy = pltpu.make_async_copy(source, target, load_sem.at[number])
        copy.start()
        return copy

    def link_part(ref, mu):
        size = ref.shape[0] // 4
        return ref.at[pl.ds(mu * size, size), :]

    load_it = load(0, it_hbm, itv)
    load_x = load(1, link_part(ga_hbm, 2), link_part(ga, 2))
    place = {n: lax.axis_index(n) for n in names}
    depth = counts["gz"]
    core = lax.rem(place["gz"], 2)
    several_pairs = depth > 2

    def along_z(step):
        return {"gz": lax.rem(place["gz"] + depth + step, depth)}

    def pair_of(other):
        return {"gz": place["gz"] - core + other}

    def away(name, step, other):
        return {name: lax.rem(place[name] + counts[name] + step, counts[name]), **pair_of(other)}

    ways = (("xy", -1), ("xy", 1), ("ta", -1), ("ta", 1))
    greeted = [away(name, step, other) for name, step in ways for other in range(2)]
    greeted += [along_z(step) for step in ((-1, 1, -2, 2) if several_pairs else (1,))]
    barrier = pltpu.get_barrier_semaphore()
    for target in greeted:
        pl.semaphore_signal(barrier, inc=1, device_id=target, device_id_type=MESH)
    load_t = load(2, link_part(ga_hbm, 0), link_part(ga, 0))
    load_z = load(3, link_part(ga_hbm, 1), link_part(ga, 1))
    load_bc = load(4, bc_hbm, bc_ref)
    load_slot = load(5, slot_hbm, slot_ref)

    def message(sent, arrived, source, target, device):
        return pltpu.make_async_remote_copy(
            src_ref=source, dst_ref=target, send_sem=send_sem.at[sent], recv_sem=recv_sem.at[arrived],
            device_id=device, device_id_type=MESH,
        )

    def await_bytes(sem, shaped):
        pltpu.make_async_copy(shaped, shaped, sem).wait()

    row = lax.broadcasted_iota(jnp.int32, (8, 128), 0)
    lane = lax.broadcasted_iota(jnp.int32, (8, 128), 1)
    column_y = lane & (LY - 1)
    group = lane // LY
    top = row < BLK

    def gauge(mu, t):
        return lambda ri, m: rows(ga, ((mu * 2 + ri) * 9 + m) * T + t)

    def gauge_edge_z(ri, m):
        return ga[pl.ds((((2 + ri) * 9 + m) * T) * 8 + 7, T, stride=8), :]

    def gauge_edge_x(ri, m):
        return rows(gx, ri * 9 + m)

    def site(field, t):
        return spinor_of(lambda k: rows(field, k * T + t))

    def gathered(values, offset):
        moved = [roll(v, LY * t + offset, 1) for t, v in enumerate(values)]
        value = moved[T - 1]
        for t in range(T - 1):
            value = jnp.where(group == t, moved[t], value)
        return value

    def pack_links():
        for ri in range(2):
            for m in range(9):
                base = (((4 + ri) * 9 + m) * T)
                put_rows(gx, ri * 9 + m, gathered([rows(ga, base + t) for t in range(T)], LY))

    def halo(d, number, name, outgoing, incoming, choice):
        copies = []
        for way in (choice, 1 - choice):
            target = {name: lax.rem(place[name] + counts[name] - 1 + 2 * way, counts[name])}
            copies.append(message(number + way, number + way, outgoing.at[d, way], incoming.at[d, way], target))
        return copies

    def halos(d):
        to_first = {n: (place[n] + 1) // counts[n] for n in ("xy", "ta")}
        return (
            halo(d, 0, "xy", sx, rx, to_first["xy"]),
            halo(d, 2, "ta", st, rt, lax.rem(place["ta"], 2) if d == 0 else to_first["ta"]),
            halo(d, 4, "gz", sz, rz, 0),
        )

    def start_all(copies):
        for copy in copies:
            copy.start()

    def start_if(which, copies):
        @pl.when(core == which)
        def _():
            start_all(copies)

    def fill_x(d, field):
        sites = [site(field, t) for t in range(T)]

        def joined(forward, offset):
            halves = [project(psi, 2, forward) for psi in sites]
            return [
                [tuple(gathered([h[s][c][ri] for h in halves], offset) for ri in range(2)) for c in range(3)]
                for s in range(2)
            ]

        put_half(joined(True, 0), lambda c, v: put_rows(sx.at[d, 0], c, v))
        put_half(link_dagger(gauge_edge_x, joined(False, LY)), lambda c, v: put_rows(sx.at[d, 1], c, v))

    def fill_t(d, field):
        put_half(project(site(field, 0), 0, True), lambda c, v: put_rows(st.at[d, 0], c, v))
        half = link_dagger(gauge(0, T - 1), project(site(field, T - 1), 0, False))
        put_half(half, lambda c, v: put_rows(st.at[d, 1], c, v))

    def fill_z(d, field):
        low = spinor_of(lambda k: field[pl.ds(k * T * 8, T, stride=8), :])
        put_half(project(low, 1, True), lambda c, v: put_rows(sz.at[d, 0], c, v, T))
        high = spinor_of(lambda k: field[pl.ds(k * T * 8 + 7, T, stride=8), :])
        half = link_dagger(gauge_edge_z, project(high, 1, False))
        put_half(half, lambda c, v: put_rows(sz.at[d, 1], c, v, T))

    def local_part(field, base, out, sign_y, before, later, moved=None):
        def keep(total, t, old):
            for s in range(4):
                for c in range(3):
                    for ri in range(2):
                        at = (ri * 12 + s * 3 + c) * T + t
                        value = 0.5 * total[s][c][ri]
                        put_rows(out, at, rows(out, at) + value if old else value)

        def inside_tile(t, carry):
            psi = site(field, t)
            total = zero_spinor(psi[0][0][0])
            inner = map_half(project(psi, 2, True), lambda v: jnp.where(lane >= 128 - LY, 0.0, roll(v, -LY, 1)))
            rebuild(total, link_times(gauge(2, t), inner), 2, True)
            inner = link_dagger(gauge(2, t), project(psi, 2, False))
            rebuild(total, map_half(inner, lambda v: jnp.where(lane < LY, 0.0, roll(v, LY, 1))), 2, False)
            inner = map_half(project(psi, 1, True), lambda v: jnp.where(row == 7, 0.0, roll(v, -1, 0)))
            rebuild(total, link_times(gauge(1, t), inner), 1, True)
            inner = link_dagger(gauge(1, t), project(psi, 1, False))
            rebuild(total, map_half(inner, lambda v: jnp.where(row == 0, 0.0, roll(v, 1, 0))), 1, False)
            keep(total, t, False)
            return carry

        lax.fori_loop(0, T, inside_tile, 0)
        before[0]()

        def along_t_y(t, carry):
            total = zero_spinor(lane.astype(F32))
            next_t, last_t = lax.rem(t + 1, T), lax.rem(t + T - 1, T)
            inside = jnp.where(t == T - 1, 0.0, 1.0)
            inner = link_times(gauge(0, t), project(site(field, next_t), 0, True))
            rebuild(total, map_half(inner, lambda v: v * inside), 0, True)
            within = jnp.where(t == 0, 0.0, 1.0)
            inner = link_dagger(gauge(0, last_t), project(site(field, last_t), 0, False))
            rebuild(total, map_half(inner, lambda v: v * within), 0, False)
            psi = site(field, t)

            def up(v):
                return jnp.where(column_y == LY - 1, roll(v, LY - 1, 1) * sign_y, roll(v, -1, 1))

            def down(v):
                return jnp.where(column_y == 0, roll(v, 1 - LY, 1) * sign_y, roll(v, 1, 1))

            rebuild(total, link_times(gauge(3, t), map_half(project(psi, 3, True), up)), 3, True)
            rebuild(total, map_half(link_dagger(gauge(3, t), project(psi, 3, False)), down), 3, False)
            keep(total, t, True)
            return carry

        lax.fori_loop(0, T, along_t_y, 0)
        before[1]()
        later()

        def on_site(t, carry):
            psi = site(field, t)
            for ch in range(2):
                for i in range(6):
                    s, c = 2 * ch + i // 3, i % 3
                    re, im = psi[s][c][0] * MASS_TERM, psi[s][c][1] * MASS_TERM
                    for j in range(6):
                        vr, vi = psi[2 * ch + j // 3][j % 3]
                        index = (ch * 2 * 36 + i * 6 + j) * T + t
                        mr, mi = rows(cl, index), rows(cl, index + 36 * T)
                        re = re + (mr * vr - mi * vi)
                        im = im + (mr * vi + mi * vr)
                    k = s * 3 + c
                    here, there = k * T + t, (12 + k) * T + t
                    put_rows(out, here, rows(out, here) + rows(base, here) - re)
                    put_rows(out, there, rows(out, there) + rows(base, there) - im)
                    if moved is not None:
                        for at, value in ((here, psi[s][c][0]), (there, psi[s][c][1])):
                            put_rows(moved, at, rows(itv, at) + value)
            return carry

        lax.fori_loop(0, T, on_site, 0)

    def add_to(out, total, where):
        for s in range(4):
            for c in range(3):
                for ri in range(2):
                    spot = where(ri * 12 + s * 3 + c)
                    out[spot] = out[spot] + 0.5 * total[s][c][ri]

    def wait_all(copies):
        for copy in copies:
            copy.wait()

    def far_part(d, out, copies, last, first):
        wait_all(copies[2])
        edge = half_of(lambda c: rows(rz.at[d, 0], c, T) * last[1])
        total = zero_spinor(edge[0][0][0])
        rebuild(total, link_times(gauge_edge_z, edge), 1, True)
        add_to(out, total, lambda k: (pl.ds(k * T * 8 + 7, T, stride=8), slice(None)))
        total = zero_spinor(edge[0][0][0])
        rebuild(total, half_of(lambda c: rows(rz.at[d, 1], c, T) * first[1]), 1, False)
        add_to(out, total, lambda k: (pl.ds(k * T * 8, T, stride=8), slice(None)))
        wait_all(copies[1])
        total = zero_spinor(lane.astype(F32))
        edge = half_of(lambda c: rows(rt.at[d, 0], c) * last[0])
        rebuild(total, link_times(gauge(0, T - 1), edge), 0, True)
        add_to(out, total, lambda k: (pl.ds((k * T + T - 1) * 8, 8), slice(None)))
        total = zero_spinor(lane.astype(F32))
        rebuild(total, half_of(lambda c: rows(rt.at[d, 1], c) * first[0]), 0, False)
        add_to(out, total, lambda k: (pl.ds(k * T * 8, 8), slice(None)))
        wait_all(copies[0])
        edge = half_of(lambda c: rows(rx.at[d, 0], c) * last[2])
        put_half(link_times(gauge_edge_x, edge), lambda c, v: put_rows(hx, c, v))
        way = jnp.where(group == T - 1, -1.0, 1.0)
        for t in range(T):
            def both(c):
                fore = roll(rows(hx, c), -LY * (t + 1), 1)
                back = roll(rows(rx.at[d, 1], c) * first[2], -LY * t, 1)
                return jnp.where(group == T - 1, fore, jnp.where(group == 0, back, 0.0))

            half = half_of(both)
            total = zero_spinor(lane.astype(F32))
            for s in range(2):
                index, power = LOWER[2][s]
                for c in range(3):
                    total[s][c] = half[s][c]
                    z = half[index][c]
                    total[2 + s][c] = add_turned(total[2 + s][c], (z[0] * way, z[1] * way), power)
            add_to(out, total, lambda k: (pl.ds((k * T + t) * 8, 8), slice(None)))

    load_it.wait()
    load_cl = load(0, cl_hbm, cl)
    load_x.wait()
    load_y = load(1, link_part(ga_hbm, 3), link_part(ga, 3))
    pack_links()
    fill_x(0, itv)
    load_t.wait()
    load_src = load(2, src_hbm, src)
    fill_t(0, itv)
    load_z.wait()
    load_co = load(3, co_hbm, co)
    fill_z(0, itv)
    load_bc.wait()
    load_nu = load(4, nu_hbm, nu)
    load_slot.wait()
    red[...] = jnp.zeros(red.shape, F32)
    pl.semaphore_wait(barrier, len(greeted))
    copies = halos(0)
    for group_of in copies:
        start_all(group_of)
    sign = [bc_ref[mu].astype(F32) for mu in range(4)]
    last = [jnp.where(place[n] == counts[n] - 1, sign[i], 1.0) for i, n in enumerate(names)]
    first = [jnp.where(place[n] == 0, sign[i], 1.0) for i, n in enumerate(names)]
    swap = jnp.full((8, 128), slot_ref[0], jnp.int32) != 0

    def ready_site():
        load_src.wait()
        load_cl.wait()

    nothing = lambda: None
    local_part(itv, src, res, sign[3], (load_y.wait, ready_site), nothing)

    def pack_coarse(k, carry):
        for i in range(nv):
            parts = [co[k, ri, i, col] for col in range(2) for ri in range(2)]
            parts = [jnp.concatenate([v, jnp.zeros((8, 128 - nv), F32)], axis=1) for v in parts]
            value = parts[0]
            for g in range(1, 4):
                value = value + roll(parts[g], LANES * g, 1)
            pk[k, i] = value
        return carry

    load_co.wait()
    lax.fori_loop(0, 9, pack_coarse, 0)

    @pl.when(core == 0)
    def _():
        message(6, 8, pk, pks, pair_of(1)).start()

    far_part(0, res, copies, last, first)

    def to_columns(k):
        low, high = [], []
        for pair, group_of in enumerate((low, high)):
            a, b = rows(res, k * T + 2 * pair), rows(res, k * T + 2 * pair + 1)
            col_0, col_1 = split_columns(a, b, top)
            group_of.append(jnp.where(swap, col_1, col_0))
            group_of.append(jnp.where(swap, col_0, col_1))
        for slot in range(2):
            value = jnp.concatenate([low[slot], high[slot]], axis=0).astype(jnp.bfloat16)
            fc[slot, k] = value
            fc[slot, 24 + k] = -value

    several(24, 4, to_columns)
    load_nu.wait()
    for slot in range(2):
        def restrict(g):
            sums = [None] * 4
            for s in range(12):
                fr, fi, minus = fc[slot, s], fc[slot, 12 + s], fc[slot, 24 + s]
                for j in range(2):
                    nr, ni = nu[slot, 0, g * 2 + j, s], nu[slot, 1, g * 2 + j, s]
                    for q, pair in enumerate(((fr, fi), (fi, minus))):
                        at = 2 * j + q
                        term = wide(nr, pair[0])
                        sums[at] = term if sums[at] is None else sums[at] + term
                        sums[at] = sums[at] + wide(ni, pair[1])
            for j in range(2):
                for ri in range(2):
                    value = sums[2 * j + ri]
                    put_rows(red, (2 * slot + ri) * LANES + g * 2 + j, value[:8] + value[8:])

        several(nv // 2, 4, restrict)
    gathered_rows = red[pl.ds(0, 128, stride=8), :]
    for r in range(1, 8):
        gathered_rows = gathered_rows + red[pl.ds(r, 128, stride=8), :]
    turned = jnp.transpose(gathered_rows)
    value = None
    for m in range(4):
        part_sum = turned[8 * m:8 * m + 8]
        for x in range(1, BLK):
            part_sum = part_sum + turned[LY * x + 8 * m:LY * x + 8 * m + 8]
        part_sum = part_sum + roll(part_sum, 1, 0)
        part_sum = part_sum + roll(part_sum, 2, 0)
        lower, upper = roll(part_sum, 2 * m - 3, 0), roll(part_sum, 2 * m + 1 - 7, 0)
        here = jnp.where(row == 2 * m, lower, upper)
        value = here if m == 0 else jnp.where(row // 2 == m, here, value)
    value = jnp.where(swap, roll(value, 2 * LANES, 1), value)
    rh[1] = value
    wone[...] = RELAX_WEIGHT * value
    for d, (name, step) in enumerate(ways):
        message(0, 6 + 4 * core, wone, wr0.at[core, d], away(name, step, 1)).start()
    if several_pairs:
        message(7, 13, wone, zr.at[0, 1 - core], along_z(3 * core - 1)).start()

    even = (group & 1) == 0
    turn = jnp.where(even, 1.0, -1.0)
    half = 2 * LANES
    block = 8

    def pairs_of(w):
        return w * turn, jnp.where(even, roll(w, -LANES, 1), roll(w, LANES, 1))

    def products(table, vectors, i, sums):
        for k, (wa, wb) in vectors:
            y = table[k, i]
            sums = (y * wa, y * wb) if sums is None else (sums[0] + y * wa, sums[1] + y * wb)
        return sums

    def near(table, own, above, below, h):
        turned = roll(own, half, 1)
        next_z = jnp.where(lane < half, turned, roll(above, half, 1))
        last_z = jnp.where(lane < half, roll(below, half, 1), turned)
        places = ((0, own), (7, roll(own, -1, 0)), (8, roll(own, 1, 0)), (3, next_z), (4, last_z))
        vectors = [(k, pairs_of(w)) for k, w in places]

        def body(g, carry):
            for j in range(block):
                i = g * block + j
                part[h, 0, i], part[h, 1, i] = products(table, vectors, i, None)
            return carry

        lax.fori_loop(0, nv // block, body, 0)

    def far(table, arrived, own, known, h):
        vectors = [(k, pairs_of(arrived[d])) for k, d in ((1, 2), (2, 3), (5, 0), (6, 1))]
        applied = jnp.zeros((8, 128), F32)
        for i in range(nv):
            sums = products(table, vectors, i, (part[h, 0, i], part[h, 1, i]))
            for ri in range(2):
                for col in range(2):
                    mine = (lane < half) if col == 0 else (lane >= half)
                    whole = jnp.sum(jnp.where(mine, sums[ri], 0.0), axis=1, keepdims=True)
                    applied = jnp.where(lane == LANES * (2 * col + ri) + i, whole, applied)
        return own + RELAX_WEIGHT * (known - (2.0 * own + applied))

    @pl.when(core == 0)
    def _():
        message(0, 7, rh.at[1], rh.at[0], pair_of(1)).start()

    @pl.when(core == 1)
    def _():
        tables = (pks, pk)
        await_bytes(recv_sem.at[7], rh.at[0])
        wmid[0, 0] = RELAX_WEIGHT * rh[0]
        wmid[0, 1] = wone[...]
        await_bytes(recv_sem.at[8], pks)
        for it in range(2):
            lower, upper = wmid[it, 0], wmid[it, 1]
            below, above = upper, lower
            if several_pairs:
                await_bytes(recv_sem.at[13 + it], zr.at[it])
                below, above = zr[it, 0], zr[it, 1]
            near(tables[1], upper, above, lower, 1)
            near(tables[0], lower, upper, below, 0)
            for h in (1, 0):
                source = wr0 if it == 0 else wr1
                await_bytes(recv_sem.at[(6, 10)[h] if it == 0 else (9, 11)[h]], source.at[h])
                wmid[it + 1, h] = far(tables[h], [source[h, d] for d in range(4)], wmid[it, h], rh[h], h)
                done = wmid.at[it + 1, h]
                for d, (name, step) in enumerate(ways):
                    if it == 0:
                        message(0, (9, 11)[h], done, wr1.at[h, d], away(name, step, 1)).start()
                    else:
                        message(0, 12, done, wr2.at[d], away(name, step, h)).start()
                if several_pairs:
                    if it == 0:
                        message(7, 14, done, zr.at[1, 1 - h], along_z(4 * h - 2)).start()
                    else:
                        message(7, 15, done, zfin, along_z(3 * h - 2)).start()
        message(0, 7, wmid.at[2], fin, pair_of(0)).start()
        fin[0] = wmid[2, 1]
        fin[1] = wmid[2, 0]

    @pl.when(core == 0)
    def _():
        await_bytes(recv_sem.at[7], fin)

    own, above, below = fin[0], fin[1], fin[1]
    if several_pairs:
        await_bytes(recv_sem.at[15], zfin)
        above, below = jnp.where(core == 0, above, zfin[...]), jnp.where(core == 0, zfin[...], below)
    near(pk, own, above, below, 0)
    await_bytes(recv_sem.at[12], wr2)
    w = far(pk, [wr2[d] for d in range(4)], own, rh[1], 0)

    @pl.when(core == 0)
    def _():
        await_bytes(send_sem.at[0], pk.at[0, pl.ds(0, 5)])
        await_bytes(send_sem.at[6], pk)
        if several_pairs:
            await_bytes(send_sem.at[7], wone)

    @pl.when(core == 1)
    def _():
        await_bytes(send_sem.at[0], pk.at[0, pl.ds(0, 22)])
        if several_pairs:
            await_bytes(send_sem.at[7], pk.at[0, pl.ds(0, 5)])

    w = jnp.where(swap, roll(w, 2 * LANES, 1), w)
    tall = []
    for m in range(4):
        low, high = jnp.broadcast_to(w[2 * m:2 * m + 1], (8, 128)), jnp.broadcast_to(w[2 * m + 1:2 * m + 2], (8, 128))
        tall.append(jnp.where(top, low, high))
    wexp[...] = jnp.transpose(jnp.concatenate(tall * BLK, axis=0))

    def spread(c):
        for slot in range(2):
            values = [wexp[pl.ds((2 * slot + ri) * LANES + c, 1), :] for ri in range(2)]
            for at, v in enumerate((values[0], values[1], -values[1])):
                wv[slot, at, c] = jnp.broadcast_to(v, (2 * 8, 128)).astype(jnp.bfloat16)

    several(nv, 4, spread)
    for slot in range(2):
        def prolong(q, carry):
            sums = [None] * 4
            for c in range(nv):
                vr, vi, minus = wv[slot, 0, c], wv[slot, 1, c], wv[slot, 2, c]
                for j in range(2):
                    nr, ni = nu[slot, 0, c, q * 2 + j], nu[slot, 1, c, q * 2 + j]
                    for ri, pair in enumerate(((vr, minus), (vi, vr))):
                        at = 2 * j + ri
                        term = wide(nr, pair[0])
                        sums[at] = term if sums[at] is None else sums[at] + term
                        sums[at] = sums[at] + wide(ni, pair[1])
            for j in range(2):
                for ri in range(2):
                    pc[slot, ri * 12 + q * 2 + j] = sums[2 * j + ri]
            return carry

        lax.fori_loop(0, 6, prolong, 0)

    def from_columns(k):
        for pair in range(2):
            part_0, part_1 = pc[0, k, pl.ds(8 * pair, 8), :], pc[1, k, pl.ds(8 * pair, 8), :]
            part_0, part_1 = jnp.where(swap, part_1, part_0), jnp.where(swap, part_0, part_1)
            for h, value in enumerate(split_columns(part_0, part_1, top)):
                at = k * T + 2 * pair + h
                put_rows(corr, at, value)

    several(24, 4, from_columns)
    copies = halos(1)
    fill_x(1, corr)
    start_if(0, copies[0])
    fill_t(1, corr)
    start_if(0, copies[1])
    fill_z(1, corr)
    start_all(copies[2])
    local_part(corr, res, out_res, sign[3], (nothing,) * 2, lambda: start_if(1, copies[0] + copies[1]), out_it)
    far_part(1, out_res, copies, last, first)


def hand_over(it_in, res_in, it_out, res_out, sem):
    copies = [
        pltpu.make_async_copy(a, b, sem.at[i]) for i, (a, b) in enumerate(((it_in, it_out), (res_in, res_out)))
    ]
    for copy in copies:
        copy.start()
    for copy in copies:
        copy.wait()


def per_device(counts, source, iterate, gauge_links, clover, bc_sign, null_store, block_slot, coarse_links):
    lattice = source.shape[3:]
    T = lattice[0]
    columns = block_slot.size
    nv = null_store.shape[4]
    assert lattice == (BLK, 2 * BLK, BLK * LY) and columns == 2 and nv % 8 == 0 and nv <= LANES
    nulls = (columns,) + null_store.shape[3:6] + (BLK * BLK, BLK * LY)
    links = jnp.transpose(coarse_links, (0, 1, 2, 4, 5, 6, 7, 3))
    links = links.reshape(links.shape[:3] + (columns,) + links.shape[6:])
    tall = T * lattice[1]
    field = (24 * tall, lattice[2])
    half = 12 * lattice[1]
    tile = lattice[1:]
    hbm = pl.BlockSpec(memory_space=pltpu.HBM)
    vmem = pl.BlockSpec(memory_space=pltpu.VMEM)
    outs = pl.pallas_call(
        functools.partial(kernel, counts),
        out_shape=(pltpu.VMEM(field, F32),) * 2,
        in_specs=[hbm] * 8,
        out_specs=(vmem,) * 2,
        scratch_shapes=[
            pltpu.SMEM(bc_sign.shape, jnp.int32),
            pltpu.SMEM((columns,), jnp.int32),
            pltpu.VMEM(field, F32),
            pltpu.VMEM(field, F32),
            pltpu.VMEM((72 * tall, 128), F32),
            pltpu.VMEM((144 * tall, 128), F32),
            pltpu.VMEM(nulls, jnp.bfloat16),
            pltpu.VMEM(links.shape, F32),
            pltpu.VMEM(field, F32),
            pltpu.VMEM(field, F32),
            pltpu.VMEM((18 * 8, 128), F32),
            pltpu.VMEM((2, 2, half, 128), F32),
            pltpu.VMEM((2, 2, half, 128), F32),
            pltpu.VMEM((2, 2, 12 * T, 128), F32),
            pltpu.VMEM((2, 2, half, 128), F32),
            pltpu.VMEM((2, 2, half, 128), F32),
            pltpu.VMEM((2, 2, 12 * T, 128), F32),
            pltpu.VMEM((half, 128), F32),
            pltpu.VMEM((columns, 48, BLK * BLK, 128), jnp.bfloat16),
            pltpu.VMEM((128 * 8, 128), F32),
            pltpu.VMEM((9, nv) + tile, F32),
            pltpu.VMEM((9, nv) + tile, F32),
            pltpu.VMEM((2, 2, nv) + tile, F32),
            pltpu.VMEM(tile, F32),
            pltpu.VMEM((2,) + tile, F32),
            pltpu.VMEM((2, 4) + tile, F32),
            pltpu.VMEM((2, 4) + tile, F32),
            pltpu.VMEM((4,) + tile, F32),
            pltpu.VMEM((3, 2) + tile, F32),
            pltpu.VMEM((2,) + tile, F32),
            pltpu.VMEM((2, 2) + tile, F32),
            pltpu.VMEM(tile, F32),
            pltpu.VMEM((128, 128), F32),
            pltpu.VMEM((columns, 3, nv, BLK * BLK, 128), jnp.bfloat16),
            pltpu.VMEM((columns, 24, BLK * BLK, 128), F32),
            pltpu.SemaphoreType.DMA((6,)),
            pltpu.SemaphoreType.DMA((8 if counts["gz"] > 2 else 7,)),
            pltpu.SemaphoreType.DMA((16 if counts["gz"] > 2 else 13,)),
        ],
        compiler_params=pltpu.CompilerParams(
            collective_id=0, has_side_effects=True, vmem_limit_bytes=66_200_000
        ),
    )(
        bc_sign,
        block_slot.reshape(-1),
        source.reshape(field),
        iterate.reshape(field),
        gauge_links.reshape(72 * tall, 128),
        clover.reshape(144 * tall, 128),
        null_store.reshape(nulls),
        links,
    )
    outs = [pltpu.with_memory_space_constraint(out, pltpu.VMEM) for out in outs]
    outs = pl.pallas_call(
        hand_over,
        out_shape=(jax.ShapeDtypeStruct(field, F32),) * 2,
        in_specs=[vmem] * 2,
        out_specs=(hbm,) * 2,
        scratch_shapes=[pltpu.SemaphoreType.DMA((2,))],
        compiler_params=pltpu.CompilerParams(vmem_limit_bytes=66_200_000),
    )(*outs)
    return tuple(out.reshape(source.shape) for out in outs)


def solution(mesh):
    placed = (
        P(None, None, None, "ta", "gz", "xy"),
        P(None, None, None, "ta", "gz", "xy"),
        P(None, None, None, None, "ta", "gz", "xy"),
        P(None, None, None, None, "ta", "gz", "xy"),
        P(),
        P("ta", "gz", "xy", None, None, None, None, None, None),
        P("ta", "gz", "xy"),
        P(None, None, None, None, "ta", "gz", "xy", None),
    )
    return jax.shard_map(
        functools.partial(per_device, dict(mesh.shape)),
        mesh=mesh,
        in_specs=placed,
        out_specs=(P(None, None, None, "ta", "gz", "xy"), P(None, None, None, "ta", "gz", "xy")),
        check_vma=False,
    )
```

```python
import functools

import jax
import jax.numpy as jnp
from jax import lax
from jax.experimental import pallas as pl
from jax.experimental.pallas import tpu as pltpu
from jax.sharding import PartitionSpec as P

BLK = 4
LY = 32
MASS_TERM = 3.8
RELAX_WEIGHT = 0.4
MESH = pl.DeviceIdType.MESH
LANES = 32
F32 = jnp.float32

UPPER = [((0, 0), (1, 0)), ((0, 3), (1, 1)), ((1, 3), (0, 3)), ((1, 2), (0, 0))]
LOWER = [((0, 0), (1, 0)), ((0, 1), (1, 3)), ((1, 1), (0, 1)), ((1, 0), (0, 2))]


def add_turned(a, b, power):
    power %= 4
    if power == 0:
        return (a[0] + b[0], a[1] + b[1])
    if power == 1:
        return (a[0] - b[1], a[1] + b[0])
    if power == 2:
        return (a[0] - b[0], a[1] - b[1])
    return (a[0] + b[1], a[1] - b[0])


def project(psi, mu, forward):
    turn = 2 if forward else 0
    return [
        [add_turned(psi[row][c], psi[2 + UPPER[mu][row][0]][c], UPPER[mu][row][1] + turn) for c in range(3)]
        for row in range(2)
    ]


def rebuild(total, half, mu, forward):
    turn = 2 if forward else 0
    for row in range(2):
        index, power = LOWER[mu][row]
        for c in range(3):
            total[row][c] = add_turned(total[row][c], half[row][c], 0)
            total[2 + row][c] = add_turned(total[2 + row][c], half[index][c], power + turn)


def link_times(link, half):
    out = [[None] * 3 for _ in range(2)]
    for a in range(3):
        for b in range(3):
            ur, ui = link(0, a * 3 + b), link(1, a * 3 + b)
            for s in range(2):
                hr, hi = half[s][b]
                term = (ur * hr - ui * hi, ur * hi + ui * hr)
                out[s][a] = term if b == 0 else add_turned(out[s][a], term, 0)
    return out


def link_dagger(link, half):
    out = [[None] * 3 for _ in range(2)]
    for a in range(3):
        for b in range(3):
            ur, ui = link(0, b * 3 + a), link(1, b * 3 + a)
            for s in range(2):
                hr, hi = half[s][b]
                term = (ur * hr + ui * hi, ur * hi - ui * hr)
                out[s][a] = term if b == 0 else add_turned(out[s][a], term, 0)
    return out


def rows(ref, index, height=8):
    start = index * height
    return ref[pl.ds(start if isinstance(index, int) else pl.multiple_of(start, height), height), :]


def put_rows(ref, index, value, height=8):
    start = index * height
    ref[pl.ds(start if isinstance(index, int) else pl.multiple_of(start, height), height), :] = value


def spinor_of(get):
    return [[(get(s * 3 + c), get(12 + s * 3 + c)) for c in range(3)] for s in range(4)]


def half_of(get):
    return [[(get(s * 3 + c), get(6 + s * 3 + c)) for c in range(3)] for s in range(2)]


def put_half(half, put):
    for s in range(2):
        for c in range(3):
            put(s * 3 + c, half[s][c][0])
            put(6 + s * 3 + c, half[s][c][1])


def map_half(half, change):
    return [[(change(z[0]), change(z[1])) for z in row] for row in half]


def zero_spinor(like):
    return [[(jnp.zeros_like(like), jnp.zeros_like(like)) for _ in range(3)] for _ in range(4)]


def roll(value, shift, axis):
    shift %= value.shape[axis]
    return value if shift == 0 else pltpu.roll(value, shift, axis)


def split_columns(a, b, top):
    return (
        jnp.where(top, a, pltpu.roll(b, BLK, 0)),
        jnp.where(top, pltpu.roll(a, BLK, 0), b),
    )


def wide(a, b):
    return a.astype(F32) * b.astype(F32)


def several(count, step, work):
    def body(g, carry):
        for j in range(step):
            work(g * step + j)
        return carry

    lax.fori_loop(0, count // step, body, 0)


def kernel(
    counts, bc_hbm, slot_hbm, src_hbm, it_hbm, ga_hbm, cl_hbm, nu_hbm, co_hbm, out_it, out_res,
    bc_ref, slot_ref, src, itv, ga, cl, nu, co, res, corr, gx, st, sx, sz, rt, rx, rz, hx, fc, red, pk, pks, part, wone,
    rh, wr0, wr1, wr2, wmid, fin, zr, zfin, wexp, wv, pc, load_sem, send_sem, recv_sem,
):
    T = BLK
    names = ("ta", "gz", "xy")
    nv = nu.shape[2]

    def load(number, source, target):
        copy = pltpu.make_async_copy(source, target, load_sem.at[number])
        copy.start()
        return copy

    def link_part(ref, mu):
        size = ref.shape[0] // 4
        return ref.at[pl.ds(mu * size, size), :]

    load_it = load(0, it_hbm, itv)
    load_x = load(1, link_part(ga_hbm, 2), link_part(ga, 2))
    place = {n: lax.axis_index(n) for n in names}
    depth = counts["gz"]
    core = lax.rem(place["gz"], 2)
    several_pairs = depth > 2

    def along_z(step):
        return {"gz": lax.rem(place["gz"] + depth + step, depth)}

    def pair_of(other):
        return {"gz": place["gz"] - core + other}

    def away(name, step, other):
        return {name: lax.rem(place[name] + counts[name] + step, counts[name]), **pair_of(other)}

    ways = (("xy", -1), ("xy", 1), ("ta", -1), ("ta", 1))
    greeted = [away(name, step, other) for name, step in ways for other in range(2)]
    greeted += [along_z(step) for step in ((-1, 1, -2, 2) if several_pairs else (1,))]
    barrier = pltpu.get_barrier_semaphore()
    for target in greeted:
        pl.semaphore_signal(barrier, inc=1, device_id=target, device_id_type=MESH)
    load_t = load(2, link_part(ga_hbm, 0), link_part(ga, 0))
    load_z = load(3, link_part(ga_hbm, 1), link_part(ga, 1))
    load_bc = load(4, bc_hbm, bc_ref)
    load_slot = load(5, slot_hbm, slot_ref)

    def message(sent, arrived, source, target, device):
        return pltpu.make_async_remote_copy(
            src_ref=source, dst_ref=target, send_sem=send_sem.at[sent], recv_sem=recv_sem.at[arrived],
            device_id=device, device_id_type=MESH,
        )

    def await_bytes(sem, shaped):
        pltpu.make_async_copy(shaped, shaped, sem).wait()

    row = lax.broadcasted_iota(jnp.int32, (8, 128), 0)
    lane = lax.broadcasted_iota(jnp.int32, (8, 128), 1)
    column_y = lane & (LY - 1)
    group = lane // LY
    top = row < BLK

    def gauge(mu, t):
        return lambda ri, m: rows(ga, ((mu * 2 + ri) * 9 + m) * T + t)

    def gauge_edge_z(ri, m):
        return ga[pl.ds((((2 + ri) * 9 + m) * T) * 8 + 7, T, stride=8), :]

    def gauge_edge_x(ri, m):
        return rows(gx, ri * 9 + m)

    def site(field, t):
        return spinor_of(lambda k: rows(field, k * T + t))

    def gathered(values, offset):
        moved = [roll(v, LY * t + offset, 1) for t, v in enumerate(values)]
        value = moved[T - 1]
        for t in range(T - 1):
            value = jnp.where(group == t, moved[t], value)
        return value

    def pack_links():
        for ri in range(2):
            for m in range(9):
                base = (((4 + ri) * 9 + m) * T)
                put_rows(gx, ri * 9 + m, gathered([rows(ga, base + t) for t in range(T)], LY))

    def halo(d, number, name, outgoing, incoming, choice):
        copies = []
        for way in (choice, 1 - choice):
            target = {name: lax.rem(place[name] + counts[name] - 1 + 2 * way, counts[name])}
            copies.append(message(number + way, number + way, outgoing.at[d, way], incoming.at[d, way], target))
        return copies

    def halos(d):
        to_first = {n: (place[n] + 1) // counts[n] for n in ("xy", "ta")}
        return (
            halo(d, 0, "xy", sx, rx, to_first["xy"]),
            halo(d, 2, "ta", st, rt, lax.rem(place["ta"], 2) if d == 0 else to_first["ta"]),
            halo(d, 4, "gz", sz, rz, 0),
        )

    def start_all(copies):
        for copy in copies:
            copy.start()

    def start_if(which, copies):
        @pl.when(core == which)
        def _():
            start_all(copies)

    def fill_x(d, field):
        sites = [site(field, t) for t in range(T)]

        def joined(forward, offset):
            halves = [project(psi, 2, forward) for psi in sites]
            return [
                [tuple(gathered([h[s][c][ri] for h in halves], offset) for ri in range(2)) for c in range(3)]
                for s in range(2)
            ]

        put_half(joined(True, 0), lambda c, v: put_rows(sx.at[d, 0], c, v))
        put_half(link_dagger(gauge_edge_x, joined(False, LY)), lambda c, v: put_rows(sx.at[d, 1], c, v))

    def fill_t(d, field):
        put_half(project(site(field, 0), 0, True), lambda c, v: put_rows(st.at[d, 0], c, v))
        half = link_dagger(gauge(0, T - 1), project(site(field, T - 1), 0, False))
        put_half(half, lambda c, v: put_rows(st.at[d, 1], c, v))

    def fill_z(d, field):
        low = spinor_of(lambda k: field[pl.ds(k * T * 8, T, stride=8), :])
        put_half(project(low, 1, True), lambda c, v: put_rows(sz.at[d, 0], c, v, T))
        high = spinor_of(lambda k: field[pl.ds(k * T * 8 + 7, T, stride=8), :])
        half = link_dagger(gauge_edge_z, project(high, 1, False))
        put_half(half, lambda c, v: put_rows(sz.at[d, 1], c, v, T))

    def local_part(field, base, out, sign_y, before, later, moved=None):
        def keep(total, t, old):
            for s in range(4):
                for c in range(3):
                    for ri in range(2):
                        at = (ri * 12 + s * 3 + c) * T + t
                        value = 0.5 * total[s][c][ri]
                        put_rows(out, at, rows(out, at) + value if old else value)

        def inside_tile(t, carry):
            psi = site(field, t)
            total = zero_spinor(psi[0][0][0])
            inner = map_half(project(psi, 2, True), lambda v: jnp.where(lane >= 128 - LY, 0.0, roll(v, -LY, 1)))
            rebuild(total, link_times(gauge(2, t), inner), 2, True)
            inner = link_dagger(gauge(2, t), project(psi, 2, False))
            rebuild(total, map_half(inner, lambda v: jnp.where(lane < LY, 0.0, roll(v, LY, 1))), 2, False)
            inner = map_half(project(psi, 1, True), lambda v: jnp.where(row == 7, 0.0, roll(v, -1, 0)))
            rebuild(total, link_times(gauge(1, t), inner), 1, True)
            inner = link_dagger(gauge(1, t), project(psi, 1, False))
            rebuild(total, map_half(inner, lambda v: jnp.where(row == 0, 0.0, roll(v, 1, 0))), 1, False)
            keep(total, t, False)
            return carry

        lax.fori_loop(0, T, inside_tile, 0)
        before[0]()

        def along_t_y(t, carry):
            total = zero_spinor(lane.astype(F32))
            next_t, last_t = lax.rem(t + 1, T), lax.rem(t + T - 1, T)
            inside = jnp.where(t == T - 1, 0.0, 1.0)
            inner = link_times(gauge(0, t), project(site(field, next_t), 0, True))
            rebuild(total, map_half(inner, lambda v: v * inside), 0, True)
            within = jnp.where(t == 0, 0.0, 1.0)
            inner = link_dagger(gauge(0, last_t), project(site(field, last_t), 0, False))
            rebuild(total, map_half(inner, lambda v: v * within), 0, False)
            psi = site(field, t)

            def up(v):
                return jnp.where(column_y == LY - 1, roll(v, LY - 1, 1) * sign_y, roll(v, -1, 1))

            def down(v):
                return jnp.where(column_y == 0, roll(v, 1 - LY, 1) * sign_y, roll(v, 1, 1))

            rebuild(total, link_times(gauge(3, t), map_half(project(psi, 3, True), up)), 3, True)
            rebuild(total, map_half(link_dagger(gauge(3, t), project(psi, 3, False)), down), 3, False)
            keep(total, t, True)
            return carry

        lax.fori_loop(0, T, along_t_y, 0)
        before[1]()
        later()

        def on_site(t, carry):
            psi = site(field, t)
            for ch in range(2):
                for i in range(6):
                    s, c = 2 * ch + i // 3, i % 3
                    re, im = psi[s][c][0] * MASS_TERM, psi[s][c][1] * MASS_TERM
                    for j in range(6):
                        vr, vi = psi[2 * ch + j // 3][j % 3]
                        index = (ch * 2 * 36 + i * 6 + j) * T + t
                        mr, mi = rows(cl, index), rows(cl, index + 36 * T)
                        re = re + (mr * vr - mi * vi)
                        im = im + (mr * vi + mi * vr)
                    k = s * 3 + c
                    here, there = k * T + t, (12 + k) * T + t
                    put_rows(out, here, rows(out, here) + rows(base, here) - re)
                    put_rows(out, there, rows(out, there) + rows(base, there) - im)
                    if moved is not None:
                        for at, value in ((here, psi[s][c][0]), (there, psi[s][c][1])):
                            put_rows(moved, at, rows(itv, at) + value)
            return carry

        lax.fori_loop(0, T, on_site, 0)

    def add_to(out, total, where):
        for s in range(4):
            for c in range(3):
                for ri in range(2):
                    spot = where(ri * 12 + s * 3 + c)
                    out[spot] = out[spot] + 0.5 * total[s][c][ri]

    def wait_all(copies):
        for copy in copies:
            copy.wait()

    def far_part(d, out, copies, last, first):
        wait_all(copies[2])
        edge = half_of(lambda c: rows(rz.at[d, 0], c, T) * last[1])
        total = zero_spinor(edge[0][0][0])
        rebuild(total, link_times(gauge_edge_z, edge), 1, True)
        add_to(out, total, lambda k: (pl.ds(k * T * 8 + 7, T, stride=8), slice(None)))
        total = zero_spinor(edge[0][0][0])
        rebuild(total, half_of(lambda c: rows(rz.at[d, 1], c, T) * first[1]), 1, False)
        add_to(out, total, lambda k: (pl.ds(k * T * 8, T, stride=8), slice(None)))
        wait_all(copies[1])
        total = zero_spinor(lane.astype(F32))
        edge = half_of(lambda c: rows(rt.at[d, 0], c) * last[0])
        rebuild(total, link_times(gauge(0, T - 1), edge), 0, True)
        add_to(out, total, lambda k: (pl.ds((k * T + T - 1) * 8, 8), slice(None)))
        total = zero_spinor(lane.astype(F32))
        rebuild(total, half_of(lambda c: rows(rt.at[d, 1], c) * first[0]), 0, False)
        add_to(out, total, lambda k: (pl.ds(k * T * 8, 8), slice(None)))
        wait_all(copies[0])
        edge = half_of(lambda c: rows(rx.at[d, 0], c) * last[2])
        put_half(link_times(gauge_edge_x, edge), lambda c, v: put_rows(hx, c, v))
        way = jnp.where(group == T - 1, -1.0, 1.0)
        for t in range(T):
            def both(c):
                fore = roll(rows(hx, c), -LY * (t + 1), 1)
                back = roll(rows(rx.at[d, 1], c) * first[2], -LY * t, 1)
                return jnp.where(group == T - 1, fore, jnp.where(group == 0, back, 0.0))

            half = half_of(both)
            total = zero_spinor(lane.astype(F32))
            for s in range(2):
                index, power = LOWER[2][s]
                for c in range(3):
                    total[s][c] = half[s][c]
                    z = half[index][c]
                    total[2 + s][c] = add_turned(total[2 + s][c], (z[0] * way, z[1] * way), power)
            add_to(out, total, lambda k: (pl.ds((k * T + t) * 8, 8), slice(None)))

    load_it.wait()
    load_cl = load(0, cl_hbm, cl)
    load_x.wait()
    load_y = load(1, link_part(ga_hbm, 3), link_part(ga, 3))
    pack_links()
    fill_x(0, itv)
    load_t.wait()
    load_src = load(2, src_hbm, src)
    fill_t(0, itv)
    load_z.wait()
    load_co = load(3, co_hbm, co)
    fill_z(0, itv)
    load_bc.wait()
    load_nu = load(4, nu_hbm, nu)
    load_slot.wait()
    red[...] = jnp.zeros(red.shape, F32)
    pl.semaphore_wait(barrier, len(greeted))
    copies = halos(0)
    for group_of in copies:
        start_all(group_of)
    sign = [bc_ref[mu].astype(F32) for mu in range(4)]
    last = [jnp.where(place[n] == counts[n] - 1, sign[i], 1.0) for i, n in enumerate(names)]
    first = [jnp.where(place[n] == 0, sign[i], 1.0) for i, n in enumerate(names)]
    swap = jnp.full((8, 128), slot_ref[0], jnp.int32) != 0

    def ready_site():
        load_src.wait()
        load_cl.wait()

    nothing = lambda: None
    local_part(itv, src, res, sign[3], (load_y.wait, ready_site), nothing)

    def pack_coarse(k, carry):
        for i in range(nv):
            parts = [co[k, ri, i, col] for col in range(2) for ri in range(2)]
            parts = [jnp.concatenate([v, jnp.zeros((8, 128 - nv), F32)], axis=1) for v in parts]
            value = parts[0]
            for g in range(1, 4):
                value = value + roll(parts[g], LANES * g, 1)
            pk[k, i] = value
        return carry

    load_co.wait()
    lax.fori_loop(0, 9, pack_coarse, 0)

    @pl.when(core == 0)
    def _():
        message(6, 8, pk, pks, pair_of(1)).start()

    far_part(0, res, copies, last, first)

    def to_columns(k):
        low, high = [], []
        for pair, group_of in enumerate((low, high)):
            a, b = rows(res, k * T + 2 * pair), rows(res, k * T + 2 * pair + 1)
            col_0, col_1 = split_columns(a, b, top)
            group_of.append(jnp.where(swap, col_1, col_0))
            group_of.append(jnp.where(swap, col_0, col_1))
        for slot in range(2):
            value = jnp.concatenate([low[slot], high[slot]], axis=0).astype(jnp.bfloat16)
            fc[slot, k] = value
            fc[slot, 24 + k] = -value

    several(24, 4, to_columns)
    load_nu.wait()
    for slot in range(2):
        def restrict(g):
            sums = [None] * 4
            for s in range(12):
                fr, fi, minus = fc[slot, s], fc[slot, 12 + s], fc[slot, 24 + s]
                for j in range(2):
                    nr, ni = nu[slot, 0, g * 2 + j, s], nu[slot, 1, g * 2 + j, s]
                    for q, pair in enumerate(((fr, fi), (fi, minus))):
                        at = 2 * j + q
                        term = wide(nr, pair[0])
                        sums[at] = term if sums[at] is None else sums[at] + term
                        sums[at] = sums[at] + wide(ni, pair[1])
            for j in range(2):
                for ri in range(2):
                    value = sums[2 * j + ri]
                    put_rows(red, (2 * slot + ri) * LANES + g * 2 + j, value[:8] + value[8:])

        several(nv // 2, 4, restrict)
    gathered_rows = red[pl.ds(0, 128, stride=8), :]
    for r in range(1, 8):
        gathered_rows = gathered_rows + red[pl.ds(r, 128, stride=8), :]
    turned = jnp.transpose(gathered_rows)
    value = None
    for m in range(4):
        part_sum = turned[8 * m:8 * m + 8]
        for x in range(1, BLK):
            part_sum = part_sum + turned[LY * x + 8 * m:LY * x + 8 * m + 8]
        part_sum = part_sum + roll(part_sum, 1, 0)
        part_sum = part_sum + roll(part_sum, 2, 0)
        lower, upper = roll(part_sum, 2 * m - 3, 0), roll(part_sum, 2 * m + 1 - 7, 0)
        here = jnp.where(row == 2 * m, lower, upper)
        value = here if m == 0 else jnp.where(row // 2 == m, here, value)
    value = jnp.where(swap, roll(value, 2 * LANES, 1), value)
    rh[1] = value
    wone[...] = RELAX_WEIGHT * value
    for d, (name, step) in enumerate(ways):
        message(0, 6 + 4 * core, wone, wr0.at[core, d], away(name, step, 1)).start()
    if several_pairs:
        message(7, 13, wone, zr.at[0, 1 - core], along_z(3 * core - 1)).start()

    even = (group & 1) == 0
    turn = jnp.where(even, 1.0, -1.0)
    half = 2 * LANES
    block = 8

    def pairs_of(w):
        return w * turn, jnp.where(even, roll(w, -LANES, 1), roll(w, LANES, 1))

    def products(table, vectors, i, sums):
        for k, (wa, wb) in vectors:
            y = table[k, i]
            sums = (y * wa, y * wb) if sums is None else (sums[0] + y * wa, sums[1] + y * wb)
        return sums

    def near(table, own, above, below, h):
        turned = roll(own, half, 1)
        next_z = jnp.where(lane < half, turned, roll(above, half, 1))
        last_z = jnp.where(lane < half, roll(below, half, 1), turned)
        places = ((0, own), (7, roll(own, -1, 0)), (8, roll(own, 1, 0)), (3, next_z), (4, last_z))
        vectors = [(k, pairs_of(w)) for k, w in places]

        def body(g, carry):
            for j in range(block):
                i = g * block + j
                part[h, 0, i], part[h, 1, i] = products(table, vectors, i, None)
            return carry

        lax.fori_loop(0, nv // block, body, 0)

    def far(table, arrived, own, known, h):
        vectors = [(k, pairs_of(arrived[d])) for k, d in ((1, 2), (2, 3), (5, 0), (6, 1))]
        applied = jnp.zeros((8, 128), F32)
        for i in range(nv):
            sums = products(table, vectors, i, (part[h, 0, i], part[h, 1, i]))
            for ri in range(2):
                for col in range(2):
                    mine = (lane < half) if col == 0 else (lane >= half)
                    whole = jnp.sum(jnp.where(mine, sums[ri], 0.0), axis=1, keepdims=True)
                    applied = jnp.where(lane == LANES * (2 * col + ri) + i, whole, applied)
        return own + RELAX_WEIGHT * (known - (2.0 * own + applied))

    @pl.when(core == 0)
    def _():
        message(0, 7, rh.at[1], rh.at[0], pair_of(1)).start()

    @pl.when(core == 1)
    def _():
        tables = (pks, pk)
        await_bytes(recv_sem.at[7], rh.at[0])
        wmid[0, 0] = RELAX_WEIGHT * rh[0]
        wmid[0, 1] = wone[...]
        await_bytes(recv_sem.at[8], pks)
        for it in range(2):
            lower, upper = wmid[it, 0], wmid[it, 1]
            below, above = upper, lower
            if several_pairs:
                await_bytes(recv_sem.at[13 + it], zr.at[it])
                below, above = zr[it, 0], zr[it, 1]
            near(tables[1], upper, above, lower, 1)
            near(tables[0], lower, upper, below, 0)
            for h in (1, 0):
                source = wr0 if it == 0 else wr1
                await_bytes(recv_sem.at[(6, 10)[h] if it == 0 else (9, 11)[h]], source.at[h])
                wmid[it + 1, h] = far(tables[h], [source[h, d] for d in range(4)], wmid[it, h], rh[h], h)
                done = wmid.at[it + 1, h]
                for d, (name, step) in enumerate(ways):
                    if it == 0:
                        message(0, (9, 11)[h], done, wr1.at[h, d], away(name, step, 1)).start()
                    else:
                        message(0, 12, done, wr2.at[d], away(name, step, h)).start()
                if several_pairs:
                    if it == 0:
                        message(7, 14, done, zr.at[1, 1 - h], along_z(4 * h - 2)).start()
                    else:
                        message(7, 15, done, zfin, along_z(3 * h - 2)).start()
        message(0, 7, wmid.at[2], fin, pair_of(0)).start()
        fin[0] = wmid[2, 1]
        fin[1] = wmid[2, 0]

    @pl.when(core == 0)
    def _():
        await_bytes(recv_sem.at[7], fin)

    own, above, below = fin[0], fin[1], fin[1]
    if several_pairs:
        await_bytes(recv_sem.at[15], zfin)
        above, below = jnp.where(core == 0, above, zfin[...]), jnp.where(core == 0, zfin[...], below)
    near(pk, own, above, below, 0)
    await_bytes(recv_sem.at[12], wr2)
    w = far(pk, [wr2[d] for d in range(4)], own, rh[1], 0)

    @pl.when(core == 0)
    def _():
        await_bytes(send_sem.at[0], pk.at[0, pl.ds(0, 5)])
        await_bytes(send_sem.at[6], pk)
        if several_pairs:
            await_bytes(send_sem.at[7], wone)

    @pl.when(core == 1)
    def _():
        await_bytes(send_sem.at[0], pk.at[0, pl.ds(0, 22)])
        if several_pairs:
            await_bytes(send_sem.at[7], pk.at[0, pl.ds(0, 5)])

    w = jnp.where(swap, roll(w, 2 * LANES, 1), w)
    tall = []
    for m in range(4):
        low, high = jnp.broadcast_to(w[2 * m:2 * m + 1], (8, 128)), jnp.broadcast_to(w[2 * m + 1:2 * m + 2], (8, 128))
        tall.append(jnp.where(top, low, high))
    wexp[...] = jnp.transpose(jnp.concatenate(tall * BLK, axis=0))

    def spread(c):
        for slot in range(2):
            values = [wexp[pl.ds((2 * slot + ri) * LANES + c, 1), :] for ri in range(2)]
            for at, v in enumerate((values[0], values[1], -values[1])):
                wv[slot, at, c] = jnp.broadcast_to(v, (2 * 8, 128)).astype(jnp.bfloat16)

    several(nv, 4, spread)
    for slot in range(2):
        def prolong(q):
            sums = [None] * 4
            for c in range(nv):
                vr, vi, minus = wv[slot, 0, c], wv[slot, 1, c], wv[slot, 2, c]
                for j in range(2):
                    nr, ni = nu[slot, 0, c, q * 2 + j], nu[slot, 1, c, q * 2 + j]
                    for ri, pair in enumerate(((vr, minus), (vi, vr))):
                        at = 2 * j + ri
                        term = wide(nr, pair[0])
                        sums[at] = term if sums[at] is None else sums[at] + term
                        sums[at] = sums[at] + wide(ni, pair[1])
            for j in range(2):
                for ri in range(2):
                    pc[slot, ri * 12 + q * 2 + j] = sums[2 * j + ri]

        several(6, 2, prolong)

    def from_columns(k):
        for pair in range(2):
            part_0, part_1 = pc[0, k, pl.ds(8 * pair, 8), :], pc[1, k, pl.ds(8 * pair, 8), :]
            part_0, part_1 = jnp.where(swap, part_1, part_0), jnp.where(swap, part_0, part_1)
            for h, value in enumerate(split_columns(part_0, part_1, top)):
                at = k * T + 2 * pair + h
                put_rows(corr, at, value)

    several(24, 4, from_columns)
    copies = halos(1)
    fill_t(1, corr)
    start_if(0, copies[1])
    fill_x(1, corr)
    start_if(0, copies[0])
    fill_z(1, corr)
    start_all(copies[2])
    local_part(corr, res, out_res, sign[3], (nothing,) * 2, lambda: start_if(1, copies[0] + copies[1]), out_it)
    far_part(1, out_res, copies, last, first)


def hand_over(it_in, res_in, it_out, res_out, sem):
    copies = [
        pltpu.make_async_copy(a, b, sem.at[i]) for i, (a, b) in enumerate(((it_in, it_out), (res_in, res_out)))
    ]
    for copy in copies:
        copy.start()
    for copy in copies:
        copy.wait()


def per_device(counts, source, iterate, gauge_links, clover, bc_sign, null_store, block_slot, coarse_links):
    lattice = source.shape[3:]
    T = lattice[0]
    columns = block_slot.size
    nv = null_store.shape[4]
    assert lattice == (BLK, 2 * BLK, BLK * LY) and columns == 2 and nv % 8 == 0 and nv <= LANES
    nulls = (columns,) + null_store.shape[3:6] + (BLK * BLK, BLK * LY)
    links = jnp.transpose(coarse_links, (0, 1, 2, 4, 5, 6, 7, 3))
    links = links.reshape(links.shape[:3] + (columns,) + links.shape[6:])
    tall = T * lattice[1]
    field = (24 * tall, lattice[2])
    half = 12 * lattice[1]
    tile = lattice[1:]
    hbm = pl.BlockSpec(memory_space=pltpu.HBM)
    vmem = pl.BlockSpec(memory_space=pltpu.VMEM)
    outs = pl.pallas_call(
        functools.partial(kernel, counts),
        out_shape=(pltpu.VMEM(field, F32),) * 2,
        in_specs=[hbm] * 8,
        out_specs=(vmem,) * 2,
        scratch_shapes=[
            pltpu.SMEM(bc_sign.shape, jnp.int32),
            pltpu.SMEM((columns,), jnp.int32),
            pltpu.VMEM(field, F32),
            pltpu.VMEM(field, F32),
            pltpu.VMEM((72 * tall, 128), F32),
            pltpu.VMEM((144 * tall, 128), F32),
            pltpu.VMEM(nulls, jnp.bfloat16),
            pltpu.VMEM(links.shape, F32),
            pltpu.VMEM(field, F32),
            pltpu.VMEM(field, F32),
            pltpu.VMEM((18 * 8, 128), F32),
            pltpu.VMEM((2, 2, half, 128), F32),
            pltpu.VMEM((2, 2, half, 128), F32),
            pltpu.VMEM((2, 2, 12 * T, 128), F32),
            pltpu.VMEM((2, 2, half, 128), F32),
            pltpu.VMEM((2, 2, half, 128), F32),
            pltpu.VMEM((2, 2, 12 * T, 128), F32),
            pltpu.VMEM((half, 128), F32),
            pltpu.VMEM((columns, 48, BLK * BLK, 128), jnp.bfloat16),
            pltpu.VMEM((128 * 8, 128), F32),
            pltpu.VMEM((9, nv) + tile, F32),
            pltpu.VMEM((9, nv) + tile, F32),
            pltpu.VMEM((2, 2, nv) + tile, F32),
            pltpu.VMEM(tile, F32),
            pltpu.VMEM((2,) + tile, F32),
            pltpu.VMEM((2, 4) + tile, F32),
            pltpu.VMEM((2, 4) + tile, F32),
            pltpu.VMEM((4,) + tile, F32),
            pltpu.VMEM((3, 2) + tile, F32),
            pltpu.VMEM((2,) + tile, F32),
            pltpu.VMEM((2, 2) + tile, F32),
            pltpu.VMEM(tile, F32),
            pltpu.VMEM((128, 128), F32),
            pltpu.VMEM((columns, 3, nv, BLK * BLK, 128), jnp.bfloat16),
            pltpu.VMEM((columns, 24, BLK * BLK, 128), F32),
            pltpu.SemaphoreType.DMA((6,)),
            pltpu.SemaphoreType.DMA((8 if counts["gz"] > 2 else 7,)),
            pltpu.SemaphoreType.DMA((16 if counts["gz"] > 2 else 13,)),
        ],
        compiler_params=pltpu.CompilerParams(
            collective_id=0, has_side_effects=True, vmem_limit_bytes=66_200_000
        ),
    )(
        bc_sign,
        block_slot.reshape(-1),
        source.reshape(field),
        iterate.reshape(field),
        gauge_links.reshape(72 * tall, 128),
        clover.reshape(144 * tall, 128),
        null_store.reshape(nulls),
        links,
    )
    outs = [pltpu.with_memory_space_constraint(out, pltpu.VMEM) for out in outs]
    outs = pl.pallas_call(
        hand_over,
        out_shape=(jax.ShapeDtypeStruct(field, F32),) * 2,
        in_specs=[vmem] * 2,
        out_specs=(hbm,) * 2,
        scratch_shapes=[pltpu.SemaphoreType.DMA((2,))],
        compiler_params=pltpu.CompilerParams(vmem_limit_bytes=66_200_000),
    )(*outs)
    return tuple(out.reshape(source.shape) for out in outs)


def solution(mesh):
    placed = (
        P(None, None, None, "ta", "gz", "xy"),
        P(None, None, None, "ta", "gz", "xy"),
        P(None, None, None, None, "ta", "gz", "xy"),
        P(None, None, None, None, "ta", "gz", "xy"),
        P(),
        P("ta", "gz", "xy", None, None, None, None, None, None),
        P("ta", "gz", "xy"),
        P(None, None, None, None, "ta", "gz", "xy", None),
    )
    return jax.shard_map(
        functools.partial(per_device, dict(mesh.shape)),
        mesh=mesh,
        in_specs=placed,
        out_specs=(P(None, None, None, "ta", "gz", "xy"), P(None, None, None, "ta", "gz", "xy")),
        check_vma=False,
    )
```
